256 devices in a mesh: replica: 4 (over y, x), seq: 64 (over z, core).
Axes of the slice: x: 2, y: 2, z: 32, core: 2. Of those that a mesh axis runs over, the one named last changes fastest.
The devices are a block of a 4x8x32 slice.
Arguments:
- hidden_in: bfloat16 [64, 8192], P('replica'), parts along dimension 0, may hold values from -6 to 6
- w_query: bfloat16 [8192, 8192], P(None, 'seq'), may hold values from -1 to 1
- w_keyval: bfloat16 [8192, 2048], P(None, 'seq'), may hold values from -0.1875 to 0.1875
- key_cache: bfloat16 [64, 8192, 1024], P('replica', 'seq'), parts along dimension 0, may hold values from -15 to 15
- value_cache: bfloat16 [64, 8192, 1024], P('replica', 'seq'), parts along dimension 0, may hold values from -6 to 6
- lengths: int32 [64], P('replica'), parts along dimension 0, may hold values from 128 to 8191, as said below
- w_out: bfloat16 [8192, 8192], P('seq'), may hold values from -0.1875 to 0.1875
Outputs:
- attn_out: bfloat16 [64, 8192], P('replica', 'seq'), parts along dimension 0
The draws below stay inside these ranges and needn't reach their ends.
There are 4 independent parts, one for each index of `replica`. The reference program is written for one: setup_inputs(seed, part) draws one part's arguments, and reference() takes and returns one part's arrays. A program takes and returns all parts, laid end to end along the dimension named above; an argument that names none is the same for every part. Nothing has to cross between parts.
Inputs may be any that keep to these rules, and one draw needn't show every extreme that they name: The new token of sequence b is written at position lengths[b]; it attends to positions 0 to lengths[b].
All inputs are finite; a program needn't handle non-finite values.
Results may differ from the reference program's by a relative error of at most 0.013.
Values may be sent and summed in bfloat16 or wider, within the bound.
No kernel may reach another device: no remote copies, remote signals or barrier semaphores. Data moves between devices by JAX's collectives and lax.ppermute only.
A program may use at most 64 MiB of HBM per device.

```python
import math
import jax
import jax.numpy as jnp
from jax import lax

D = 8192
HEADS = 64
KV_HEADS = 8
HEAD_DIM = 128
BATCH = 16
CTX_DEV = 128
CTX = 8192


def plan_draw(key):
    lengths = jax.random.randint(jax.random.fold_in(key, 101), (BATCH,), CTX_DEV, CTX, dtype=jnp.int32)
    return lengths


def draw_lengths(key, part):
    return plan_draw(key)


def draw_hidden_in(key, part):
    base = jnp.clip(jax.random.normal(jax.random.fold_in(key, 1), (BATCH, D), jnp.float32), -6.0, 6.0)
    return base.astype(jnp.bfloat16)


def draw_w_query(key, part):
    width = HEADS * HEAD_DIM
    scale = 1.0 / math.sqrt(D)
    base = jnp.clip(jax.random.normal(key, (D, width), jnp.float32), -6.0, 6.0) * scale
    return base.astype(jnp.bfloat16)


def draw_key_cache(key, part):
    width = KV_HEADS * HEAD_DIM
    base = jnp.clip(jax.random.normal(jax.random.fold_in(key, 2), (BATCH, CTX, width), jnp.float32), -15.0, 15.0)
    return base.astype(jnp.bfloat16)


def raised(result, rng, source, target, shards_of, factor):
    def block_of(dim):
        return (jnp.arange(result.shape[dim]) // (result.shape[dim] // shards_of)).reshape((-1,) + (1,) * (result.ndim - 1 - dim))

    first = jax.random.permutation(rng, shards_of)[block_of(target)]
    other_side = (block_of(target) + shards_of // 2) % shards_of
    return jnp.where((block_of(source) == first) | (block_of(source) == other_side), factor * result, result)


def shard_levels(rng, shape, shards, low, top_value):
    gain = 1.0
    for dim, blocks in shards:
        heights = jax.random.uniform(jax.random.fold_in(jax.random.fold_in(rng, 6), dim), (blocks,), jnp.float32, low / len(shards), top_value / len(shards))
        gain = gain * jnp.repeat(jnp.exp(heights), shape[dim] // blocks).reshape((-1,) + (1,) * (len(shape) - 1 - dim))
    return gain


def normal_values(rng, shape, scale, reach, shards=(), kind=jnp.bfloat16):
    values = scale * jax.random.normal(rng, shape, jnp.float32)
    if shards:
        values = values * shard_levels(rng, shape, shards, -0.22, 0.18)
    return jnp.clip(values, -reach, reach).astype(kind)


def gaussian_with(key, shape, scale, limit, shards, heavy, kind=jnp.bfloat16):
    entries = scale * jax.random.normal(key, shape, jnp.float32)
    if shards:
        entries = entries * shard_levels(key, shape, shards, -0.22, 0.18)
    return jnp.clip(raised(entries, jax.random.fold_in(key, 3), *heavy), -limit, limit).astype(kind)


def setup_inputs(seed: int = 0, part: int = 0) -> dict:
    keys = jax.random.split(jax.random.key(seed), 8)
    part_splits = jax.random.split(jax.random.fold_in(keys[7], part), 8)
    return {
        "hidden_in": draw_hidden_in(jax.random.fold_in(jax.random.fold_in(keys[7], part), 71), part),
        "w_query": draw_w_query(jax.random.fold_in(keys[7], 71), part),
        "w_keyval": normal_values(keys[2], (D, 2 * KV_HEADS * HEAD_DIM), (D // 9) ** -0.5, 0.1875, ((1, 64),)),
        "key_cache": draw_key_cache(jax.random.fold_in(jax.random.fold_in(keys[7], part), 71), part),
        "value_cache": normal_values(part_splits[4], (BATCH, CTX, KV_HEADS * HEAD_DIM), 1.0, 6.0, ((1, 64),)),
        "lengths": draw_lengths(jax.random.fold_in(jax.random.fold_in(keys[7], part), 71), part),
        "w_out": gaussian_with(keys[6], (HEADS * HEAD_DIM, D), (HEADS * HEAD_DIM) ** -0.5, 0.1875, ((0, 64),), (0, 1, 64, 4.0)),
    }


def reference(hidden_in, w_query, w_keyval, key_cache, value_cache, lengths, w_out):
    query = jnp.dot(hidden_in, w_query, preferred_element_type=jnp.float32).astype(jnp.bfloat16)
    new_kv = jnp.dot(hidden_in, w_keyval, preferred_element_type=jnp.float32).astype(jnp.bfloat16)
    half_width = KV_HEADS * HEAD_DIM
    group_size = HEADS // KV_HEADS

    def attend(sequence):
        query_row, new_key, new_value, cached_keys, cached_values, position = sequence
        anchor = (position.astype(jnp.int32), jnp.int32(0))
        key_rows = lax.dynamic_update_slice(cached_keys, new_key[None, :], anchor)
        value_rows = lax.dynamic_update_slice(cached_values, new_value[None, :], anchor)
        query_f32 = query_row.astype(jnp.float32).reshape(KV_HEADS, group_size, HEAD_DIM)
        key_f32 = key_rows.astype(jnp.float32).reshape(CTX, KV_HEADS, HEAD_DIM)
        scores = jnp.einsum('kgd,tkd->kgt', query_f32, key_f32) / math.sqrt(HEAD_DIM)
        positions = jnp.arange(CTX, dtype=jnp.int32)
        scores = jnp.where(positions <= position, scores, -1e+30)
        largest = lax.optimization_barrier(jnp.max(scores, axis=-1))
        weights = jnp.exp(scores - largest[..., None])
        total = lax.optimization_barrier(jnp.sum(weights, axis=-1))
        rounded = lax.optimization_barrier(weights.astype(jnp.bfloat16)).astype(jnp.float32)
        value_f32 = value_rows.astype(jnp.float32).reshape(CTX, KV_HEADS, HEAD_DIM)
        summed = jnp.einsum('kgt,tkd->kgd', rounded, value_f32)
        return (summed / total[..., None]).reshape(HEADS * HEAD_DIM)
    attended = lax.map(attend, (query, new_kv[:, :half_width], new_kv[:, half_width:], key_cache, value_cache, lengths))
    attended = attended.astype(jnp.bfloat16)
    return jnp.dot(attended, w_out, preferred_element_type=jnp.float32).astype(jnp.bfloat16)
```

```python
import math

import jax
import jax.numpy as jnp
from jax import lax
from jax.sharding import PartitionSpec as P

KV_HEADS = 8
HEAD_DIM = 128
CORES = 2
NEAR = 4
EMPTY = -1e30


def same_core_groups(shards):
    return [[CORES * z + c for z in range(shards // CORES)] for c in range(CORES)]


def near_groups(shards):
    blocks = shards // CORES // NEAR
    return [
        [CORES * (NEAR * b + i) + c for i in range(NEAR)] for b in range(blocks) for c in range(CORES)
    ]


def far_groups(shards):
    blocks = shards // CORES // NEAR
    return [
        [CORES * (NEAR * b + i) + c for b in range(blocks)] for i in range(NEAR) for c in range(CORES)
    ]


def exchange(x, groups):
    return lax.all_to_all(
        x, "seq", split_axis=0, concat_axis=0, axis_index_groups=groups, tiled=True
    )


def to_partner(x, shards):
    return lax.ppermute(x, "seq", [(i, i ^ 1) for i in range(shards)])


def rounded(x):
    return lax.reduce_precision(x, exponent_bits=8, mantissa_bits=7)


def split_terms(x):
    high = rounded(x)
    middle = rounded(x - high)
    low = rounded(x - high - middle)
    return high.astype(jnp.bfloat16), middle.astype(jnp.bfloat16), low.astype(jnp.bfloat16)


def body(hidden_in, w_query, w_keyval, key_cache, value_cache, lengths, w_out):
    batch, ctx_dev, half_width = key_cache.shape
    shards = lax.axis_size("seq")
    index = lax.axis_index("seq")
    chips = shards // CORES
    heads = w_out.shape[0] // HEAD_DIM * shards
    group = heads // KV_HEADS
    group_chips = group // CORES
    f32, bf16 = jnp.float32, jnp.bfloat16

    query_part = jnp.dot(hidden_in, w_query, preferred_element_type=f32).astype(bf16)
    keyval_part = jnp.dot(hidden_in, w_keyval, preferred_element_type=f32).astype(bf16)
    kv_cols = keyval_part.shape[1]

    row = jnp.concatenate([query_part.reshape(1, 1, -1), keyval_part.reshape(1, 1, -1)], axis=2)
    width = row.shape[2]
    blocks = chips // NEAR
    far = exchange(jnp.broadcast_to(row, (blocks, 1, width)), far_groups(shards))
    near = exchange(
        jnp.broadcast_to(far[None], (NEAR, blocks, 1, width)).reshape(chips, 1, width),
        near_groups(shards),
    )
    partner = to_partner(near, shards)
    lines = jnp.stack([near, partner]).reshape(CORES, NEAR, blocks, width)
    lines = lines.transpose(2, 1, 0, 3)
    q_size = batch * HEAD_DIM
    query = lines[..., :q_size].reshape(KV_HEADS, group_chips, CORES, batch, HEAD_DIM)
    query = query.transpose(3, 0, 2, 1, 4).reshape(batch, KV_HEADS, group, HEAD_DIM)

    core = index % CORES
    kv_lines = lines[..., q_size:].reshape(chips, CORES, batch, kv_cols)
    kv_lines = jnp.where(core == 0, kv_lines, kv_lines[:, ::-1])
    kv_lines = kv_lines.reshape(2, KV_HEADS, -1, batch, kv_cols)
    own_group = index // group
    own_kv = lax.dynamic_slice_in_dim(kv_lines, own_group, 1, axis=1)[:, 0]
    own_kv = own_kv.transpose(0, 2, 1, 3).reshape(2, batch, HEAD_DIM).astype(f32)
    score_new = jnp.sum(query_part.astype(f32) * own_kv[0], axis=-1) / math.sqrt(HEAD_DIM)

    slots = index * ctx_dev + lax.broadcasted_iota(jnp.int32, (batch, ctx_dev), 1)
    used = (slots < lengths[:, None])[:, None, None, :]
    keys = key_cache.reshape(batch, ctx_dev, KV_HEADS, HEAD_DIM)
    values = value_cache.reshape(batch, ctx_dev, KV_HEADS, HEAD_DIM)
    scores = jnp.einsum("bkgd,btkd->bkgt", query, keys, preferred_element_type=f32)
    scores = jnp.where(used, scores / math.sqrt(HEAD_DIM), EMPTY)
    local_max = jnp.max(scores, axis=-1)
    weights = jnp.where(used, jnp.exp(scores - local_max[..., None]), 0.0)
    local_sum = jnp.sum(weights, axis=-1)
    local_out = jnp.einsum(
        "bkgt,btkd->bkgd", weights.astype(bf16), values, preferred_element_type=f32
    )
    some = local_sum > 0
    scale = jnp.where(some, 1.0 / jnp.where(some, local_sum, 1.0), 0.0)
    level = jnp.where(some, local_max + jnp.log(jnp.where(some, local_sum, 1.0)), EMPTY)
    local_out = local_out * scale[..., None]

    local_out = local_out.reshape(batch, KV_HEADS, CORES, group_chips, HEAD_DIM)
    level = level.reshape(batch, KV_HEADS, CORES, group_chips)
    local_out = local_out.transpose(2, 1, 3, 0, 4).reshape(CORES, chips, batch, HEAD_DIM)
    level = level.transpose(2, 1, 3, 0).reshape(CORES, chips, batch)
    got_out = to_partner(local_out[1].astype(bf16), shards).astype(f32)
    got_level = to_partner(level[1], shards)
    top = jnp.maximum(level[0], got_level)
    part_a = jnp.exp(level[0] - top)
    part_b = jnp.exp(got_level - top)
    whole = part_a + part_b
    merged = (local_out[0] * part_a[..., None] + got_out * part_b[..., None]) / whole[..., None]
    level = jnp.maximum(top + jnp.log(whole), EMPTY)
    stats = jnp.concatenate(split_terms(level), axis=1)
    stats = jnp.pad(stats, ((0, 0), (0, HEAD_DIM - stats.shape[1])))
    packet = jnp.concatenate([merged.astype(bf16).reshape(chips, -1), stats], axis=1)
    arrived = exchange(packet[:, None, :], same_core_groups(shards))[:, 0]
    outs = arrived[:, :q_size].reshape(chips, batch, HEAD_DIM).astype(f32)
    levels = arrived[:, q_size : q_size + 3 * batch].astype(f32).reshape(chips, 3, batch)
    levels = levels[:, 0] + (levels[:, 1] + levels[:, 2])
    top = jnp.maximum(jnp.max(levels, axis=0), score_new)
    factor = jnp.exp(levels - top)
    factor_new = jnp.exp(score_new - top)
    numerator = jnp.sum(outs * factor[..., None], axis=0) + factor_new[:, None] * own_kv[1]
    denominator = jnp.sum(factor, axis=0) + factor_new
    attended = (numerator / denominator[:, None]).astype(bf16)

    term = jnp.dot(attended, w_out, preferred_element_type=f32)
    term = term.reshape(batch, chips, CORES, -1)
    first, second = term[:, :, 0].swapaxes(0, 1), term[:, :, 1].swapaxes(0, 1)
    mine = jnp.where(core == 0, first, second)
    theirs = jnp.where(core == 0, second, first)
    mine = mine + to_partner(theirs.astype(bf16), shards).astype(f32)
    arrived = exchange(mine.astype(bf16), same_core_groups(shards))
    return jnp.sum(arrived.astype(f32), axis=0).astype(bf16)


def solution(mesh):
    placed = (
        P("replica", None),
        P(None, "seq"),
        P(None, "seq"),
        P("replica", "seq", None),
        P("replica", "seq", None),
        P("replica"),
        P("seq", None),
    )
    return jax.shard_map(
        body, mesh=mesh, in_specs=placed, out_specs=P("replica", "seq"), check_vma=False
    )
```

```python
import math

import jax
import jax.numpy as jnp
from jax import lax
from jax.experimental import pallas as pl
from jax.experimental.pallas import tpu as pltpu
from jax.sharding import PartitionSpec as P

KV_HEADS = 8
HEAD_DIM = 128
CORES = 2
NEAR = 4
EMPTY = -1e30
PACK_ROWS = 24
STEP_ROWS = 2
INTERPRET = False


def same_core_groups(shards):
    return [[CORES * z + c for z in range(shards // CORES)] for c in range(CORES)]


def near_groups(shards):
    blocks = shards // CORES // NEAR
    return [
        [CORES * (NEAR * b + i) + c for i in range(NEAR)] for b in range(blocks) for c in range(CORES)
    ]


def far_groups(shards):
    blocks = shards // CORES // NEAR
    return [
        [CORES * (NEAR * b + i) + c for b in range(blocks)] for i in range(NEAR) for c in range(CORES)
    ]


def exchange(x, groups):
    return lax.all_to_all(
        x, "seq", split_axis=0, concat_axis=0, axis_index_groups=groups, tiled=True
    )


def to_partner(x, shards):
    return lax.ppermute(x, "seq", [(i, i ^ 1) for i in range(shards)])


def rounded(x):
    return lax.reduce_precision(x, exponent_bits=8, mantissa_bits=7)


def split_terms(x):
    high = rounded(x)
    middle = rounded(x - high)
    low = rounded(x - high - middle)
    return high.astype(jnp.bfloat16), middle.astype(jnp.bfloat16), low.astype(jnp.bfloat16)


def project_kernel(hidden_ref, w_query_ref, w_keyval_ref, packet_ref, acc_q, acc_kv):
    step = pl.program_id(0)

    @pl.when(step == 0)
    def _():
        acc_q[...] = jnp.zeros_like(acc_q)
        acc_kv[...] = jnp.zeros_like(acc_kv)

    hidden = hidden_ref[...]
    acc_q[...] += jnp.dot(hidden, w_query_ref[...], preferred_element_type=jnp.float32)
    acc_kv[...] += lax.dot_general(
        hidden, w_keyval_ref[...], (((1,), (1,)), ((), ())), preferred_element_type=jnp.float32
    )

    @pl.when(step == pl.num_programs(0) - 1)
    def _():
        batch, cols = acc_kv.shape
        rows = batch * cols // HEAD_DIM
        keyval = acc_kv[...]
        keyval = jnp.concatenate(
            [keyval[i * rows : (i + 1) * rows] for i in range(HEAD_DIM // cols)], axis=1
        )
        filler = jnp.zeros((PACK_ROWS - batch - rows, HEAD_DIM), jnp.float32)
        packet = jnp.concatenate([acc_q[...], keyval, filler], axis=0).astype(jnp.bfloat16)
        for copy in range(packet_ref.shape[0]):
            packet_ref[copy] = packet


def project(hidden_in, w_query, w_keyval_t, copies):
    batch, width = hidden_in.shape
    cols = w_keyval_t.shape[0]
    steps = 4
    chunk = width // steps
    return pl.pallas_call(
        project_kernel,
        grid=(steps,),
        in_specs=[
            pl.BlockSpec((batch, chunk), lambda k: (0, k)),
            pl.BlockSpec((chunk, HEAD_DIM), lambda k: (k, 0)),
            pl.BlockSpec((cols, chunk), lambda k: (0, k)),
        ],
        out_specs=pl.BlockSpec((copies, PACK_ROWS, HEAD_DIM), lambda k: (0, 0, 0)),
        out_shape=jax.ShapeDtypeStruct((copies, PACK_ROWS, HEAD_DIM), jnp.bfloat16),
        scratch_shapes=[
            pltpu.VMEM((batch, HEAD_DIM), jnp.float32),
            pltpu.VMEM((batch, cols), jnp.float32),
        ],
        interpret=INTERPRET,
        name="project",
    )(hidden_in, w_query, w_keyval_t)


def attend_kernel(lengths_ref, first_ref, own_ref, partner_ref, key_ref, value_ref,
                  mine_ref, theirs_ref, level_ref, q_scr, o_scr, level_scr):
    step = pl.program_id(0)
    blocks = own_ref.shape[0] // NEAR
    batch = mine_ref.shape[1]
    ctx_dev = key_ref.shape[1]
    group = CORES * NEAR
    f32, bf16 = jnp.float32, jnp.bfloat16

    @pl.when(step == 0)
    def _():
        for g in range(blocks):
            for c, ref in enumerate((own_ref, partner_ref)):
                for i in range(NEAR):
                    row = (g * group + c * NEAR + i) * batch
                    q_scr[row : row + batch, :] = ref[i * blocks + g, :batch, :].astype(f32)
        level_scr[...] = jnp.full(level_scr.shape, EMPTY, f32)

    lanes = lax.broadcasted_iota(jnp.int32, (group * blocks, ctx_dev), 1)
    level_lanes = lax.broadcasted_iota(jnp.int32, level_scr.shape, 1)
    for j in range(STEP_ROWS):
        b = step * STEP_ROWS + j
        used = lanes < lengths_ref[b] - first_ref[0]
        scores = []
        for g in range(blocks):
            query = q_scr[pl.ds(g * group * batch + b, group, stride=batch), :].astype(bf16)
            keys = key_ref[j, :, g * HEAD_DIM : (g + 1) * HEAD_DIM]
            scores.append(
                lax.dot_general(
                    query, keys, (((1,), (1,)), ((), ())), preferred_element_type=f32
                )
            )
        scores = jnp.concatenate(scores, axis=0) * (1.0 / math.sqrt(HEAD_DIM))
        scores = jnp.where(used, scores, EMPTY)
        top = jnp.max(scores, axis=1, keepdims=True)
        weights = jnp.where(used, jnp.exp(scores - top), 0.0)
        total = jnp.sum(weights, axis=1, keepdims=True)
        some = total > 0
        safe = jnp.where(some, total, 1.0)
        level = jnp.where(some, top + jnp.log(safe), EMPTY)
        level_scr[...] = jnp.where(level_lanes == b, level, level_scr[...])
        inverse = 1.0 / safe
        weights = weights.astype(bf16)
        for g in range(blocks):
            rows = slice(g * group, (g + 1) * group)
            values = value_ref[j, :, g * HEAD_DIM : (g + 1) * HEAD_DIM]
            out = jnp.dot(weights[rows], values, preferred_element_type=f32) * inverse[rows]
            o_scr[pl.ds(g * group * batch + b, group, stride=batch), :] = out

    @pl.when(step == pl.num_programs(0) - 1)
    def _():
        for g in range(blocks):
            for c, ref in enumerate((mine_ref, theirs_ref)):
                for i in range(NEAR):
                    row = (g * group + c * NEAR + i) * batch
                    ref[g * NEAR + i] = o_scr[row : row + batch, :].astype(bf16)
                start = c * NEAR * blocks + g * NEAR
                source = g * group + c * NEAR
                level_ref[start : start + NEAR, :] = level_scr[source : source + NEAR, :]


def attend(lengths, first, own, partner, key_cache, value_cache):
    batch, ctx_dev, width = key_cache.shape
    chips = own.shape[0]
    heads = CORES * chips
    whole = lambda *shape: pl.BlockSpec(shape, lambda s, *_: (0,) * len(shape))
    cache = pl.BlockSpec((STEP_ROWS, ctx_dev, width), lambda s, *_: (s, 0, 0))
    return pl.pallas_call(
        attend_kernel,
        grid_spec=pltpu.PrefetchScalarGridSpec(
            num_scalar_prefetch=2,
            grid=(batch // STEP_ROWS,),
            in_specs=[whole(*own.shape), whole(*partner.shape), cache, cache],
            out_specs=[
                whole(chips, batch, HEAD_DIM),
                whole(chips, batch, HEAD_DIM),
                whole(heads, HEAD_DIM),
            ],
            scratch_shapes=[
                pltpu.VMEM((heads * batch, HEAD_DIM), jnp.float32),
                pltpu.VMEM((heads * batch, HEAD_DIM), jnp.float32),
                pltpu.VMEM((heads, HEAD_DIM), jnp.float32),
            ],
        ),
        out_shape=[
            jax.ShapeDtypeStruct((chips, batch, HEAD_DIM), jnp.bfloat16),
            jax.ShapeDtypeStruct((chips, batch, HEAD_DIM), jnp.bfloat16),
            jax.ShapeDtypeStruct((heads, HEAD_DIM), jnp.float32),
        ],
        interpret=INTERPRET,
        name="attend",
    )(lengths, first, own, partner, key_cache, value_cache)


def body(hidden_in, w_query, w_keyval, key_cache, value_cache, lengths, w_out):
    batch, ctx_dev, half_width = key_cache.shape
    shards = lax.axis_size("seq")
    index = lax.axis_index("seq")
    core = index % CORES
    chips = shards // CORES
    blocks = chips // NEAR
    heads = w_out.shape[0] // HEAD_DIM * shards
    group = heads // KV_HEADS
    kv_cols = w_keyval.shape[1]
    f32, bf16 = jnp.float32, jnp.bfloat16

    w_cols = w_out.reshape(HEAD_DIM, chips, CORES, -1)
    w_first, w_second = w_cols[:, :, 0], w_cols[:, :, 1]
    w_mine = jnp.where(core == 0, w_first, w_second).reshape(HEAD_DIM, -1)
    w_theirs = jnp.where(core == 0, w_second, w_first).reshape(HEAD_DIM, -1)
    w_partner = to_partner(w_theirs, shards)

    packet = project(hidden_in, w_query, w_keyval.T, blocks)
    far = exchange(packet, far_groups(shards))
    near = exchange(
        jnp.broadcast_to(far[None], (NEAR, *far.shape)).reshape(chips, *far.shape[1:]),
        near_groups(shards),
    )
    partner = to_partner(near, shards)

    first = (index * ctx_dev).astype(jnp.int32)[None]
    mine, theirs, level = attend(lengths, first, near, partner, key_cache, value_cache)
    level = level[:, :batch]

    rows = batch * kv_cols // HEAD_DIM
    kv = jnp.stack([near[:, batch : batch + rows], partner[:, batch : batch + rows]])
    kv = jnp.where(core == 0, kv, kv[::-1]).reshape(CORES, NEAR, blocks, rows, HEAD_DIM)
    kv = kv.transpose(2, 1, 0, 3, 4).reshape(2, KV_HEADS, -1, rows, HEAD_DIM)
    own_kv = lax.dynamic_slice_in_dim(kv, index // group, 1, axis=1)[:, 0]
    own_kv = own_kv.reshape(2, HEAD_DIM // kv_cols, rows, -1, kv_cols).transpose(0, 3, 2, 1, 4)
    own_kv = own_kv.reshape(2, batch, HEAD_DIM).astype(f32)
    query_part = packet[0, :batch].astype(f32)
    score_new = jnp.sum(query_part * own_kv[0], axis=-1) / math.sqrt(HEAD_DIM)

    got_out = to_partner(theirs, shards).astype(f32)
    got_level = to_partner(level[chips:], shards)
    level = level[:chips]
    top = jnp.maximum(level, got_level)
    part_a = jnp.exp(level - top)
    part_b = jnp.exp(got_level - top)
    whole = part_a + part_b
    merged = mine.astype(f32) * (part_a / whole)[..., None] + got_out * (part_b / whole)[..., None]
    level = jnp.maximum(top + jnp.log(whole), EMPTY)
    stats = jnp.concatenate(split_terms(level), axis=1)
    stats = jnp.pad(stats, ((0, 0), (0, HEAD_DIM - stats.shape[1])))
    sent = jnp.concatenate([merged.astype(bf16).reshape(chips, -1), stats], axis=1)
    arrived = exchange(sent[:, None, :], same_core_groups(shards))[:, 0]
    q_size = batch * HEAD_DIM
    outs = arrived[:, :q_size].reshape(chips, batch, HEAD_DIM).astype(f32)
    levels = arrived[:, q_size : q_size + 3 * batch].astype(f32).reshape(chips, 3, batch)
    levels = levels[:, 0] + (levels[:, 1] + levels[:, 2])
    top = jnp.maximum(jnp.max(levels, axis=0), score_new)
    factor = jnp.exp(levels - top)
    factor_new = jnp.exp(score_new - top)
    numerator = jnp.sum(outs * factor[..., None], axis=0) + factor_new[:, None] * own_kv[1]
    denominator = jnp.sum(factor, axis=0) + factor_new
    attended = (numerator / denominator[:, None]).astype(bf16)

    attended_partner = to_partner(attended, shards)
    term = jnp.dot(attended, w_mine, preferred_element_type=f32) + jnp.dot(
        attended_partner, w_partner, preferred_element_type=f32
    )
    term = term.astype(bf16).reshape(batch, chips, -1).swapaxes(0, 1)
    arrived = exchange(term, same_core_groups(shards))
    return jnp.sum(arrived.astype(f32), axis=0).astype(bf16)


def solution(mesh):
    placed = (
        P("replica", None),
        P(None, "seq"),
        P(None, "seq"),
        P("replica", "seq", None),
        P("replica", "seq", None),
        P("replica"),
        P("seq", None),
    )
    return jax.shard_map(
        body, mesh=mesh, in_specs=placed, out_specs=P("replica", "seq"), check_vma=False
    )
```

```python
import math

import jax
import jax.numpy as jnp
from jax import lax
from jax.experimental import pallas as pl
from jax.experimental.pallas import tpu as pltpu
from jax.sharding import PartitionSpec as P

KV_HEADS = 8
HEAD_DIM = 128
CORES = 2
NEAR = 4
EMPTY = -1e30
PACK_ROWS = 24
STEP_ROWS = 4
INTERPRET = False


def same_core_groups(shards):
    return [[CORES * z + c for z in range(shards // CORES)] for c in range(CORES)]


def near_groups(shards):
    blocks = shards // CORES // NEAR
    return [
        [CORES * (NEAR * b + i) + c for i in range(NEAR)] for b in range(blocks) for c in range(CORES)
    ]


def far_groups(shards):
    blocks = shards // CORES // NEAR
    return [
        [CORES * (NEAR * b + i) + c for b in range(blocks)] for i in range(NEAR) for c in range(CORES)
    ]


def exchange(x, groups):
    return lax.all_to_all(
        x, "seq", split_axis=0, concat_axis=0, axis_index_groups=groups, tiled=True
    )


def to_partner(x, shards):
    return lax.ppermute(x, "seq", [(i, i ^ 1) for i in range(shards)])


def rounded(x):
    return lax.reduce_precision(x, exponent_bits=8, mantissa_bits=7)


def split_terms(x):
    high = rounded(x)
    middle = rounded(x - high)
    low = rounded(x - high - middle)
    return high.astype(jnp.bfloat16), middle.astype(jnp.bfloat16), low.astype(jnp.bfloat16)


def in_vmem(x):
    return x if INTERPRET else pltpu.with_memory_space_constraint(x, pltpu.VMEM)


def in_hbm(x):
    return x if INTERPRET else pltpu.with_memory_space_constraint(x, pltpu.HBM)


def vmem_out(shape, dtype):
    return jax.ShapeDtypeStruct(shape, dtype) if INTERPRET else pltpu.VMEM(shape, dtype)


def hbm_out(shape, dtype):
    return jax.ShapeDtypeStruct(shape, dtype) if INTERPRET else pltpu.HBM(shape, dtype)


def whole():
    return pl.BlockSpec(memory_space=pltpu.VMEM)


def limit(mib):
    return pltpu.CompilerParams(vmem_limit_bytes=mib << 20)


def project_kernel(hidden_ref, w_query_ref, w_keyval_ref, packet_ref, acc_q, acc_kv):
    step = pl.program_id(0)

    @pl.when(step == 0)
    def _():
        acc_q[...] = jnp.zeros_like(acc_q)
        acc_kv[...] = jnp.zeros_like(acc_kv)

    hidden = hidden_ref[...]
    acc_q[...] += jnp.dot(hidden, w_query_ref[...], preferred_element_type=jnp.float32)
    acc_kv[...] += lax.dot_general(
        hidden, w_keyval_ref[...], (((1,), (1,)), ((), ())), preferred_element_type=jnp.float32
    )

    @pl.when(step == pl.num_programs(0) - 1)
    def _():
        batch, cols = acc_kv.shape
        rows = batch * cols // HEAD_DIM
        keyval = acc_kv[...]
        keyval = jnp.concatenate(
            [keyval[i * rows : (i + 1) * rows] for i in range(HEAD_DIM // cols)], axis=1
        )
        filler = jnp.zeros((PACK_ROWS - batch - rows, HEAD_DIM), jnp.float32)
        packet = jnp.concatenate([acc_q[...], keyval, filler], axis=0).astype(jnp.bfloat16)
        for copy in range(packet_ref.shape[0]):
            packet_ref[copy] = packet


def project(hidden_in, w_query, w_keyval_t, copies):
    batch, width = hidden_in.shape
    cols = w_keyval_t.shape[0]
    steps = 2
    chunk = width // steps
    return pl.pallas_call(
        project_kernel,
        grid=(steps,),
        in_specs=[
            pl.BlockSpec((batch, chunk), lambda k: (0, k)),
            pl.BlockSpec((chunk, HEAD_DIM), lambda k: (k, 0)),
            pl.BlockSpec((cols, chunk), lambda k: (0, k)),
        ],
        out_specs=whole(),
        out_shape=vmem_out((copies, PACK_ROWS, HEAD_DIM), jnp.bfloat16),
        scratch_shapes=[
            pltpu.VMEM((batch, HEAD_DIM), jnp.float32),
            pltpu.VMEM((batch, cols), jnp.float32),
        ],
        compiler_params=limit(8),
        interpret=INTERPRET,
        name="project",
    )(in_hbm(hidden_in), in_hbm(w_query), in_hbm(w_keyval_t))


def transpose_keys_kernel(key_ref, out_ref):
    for j in range(key_ref.shape[0]):
        for g in range(key_ref.shape[2] // HEAD_DIM):
            columns = slice(g * HEAD_DIM, (g + 1) * HEAD_DIM)
            out_ref[j, columns, :] = key_ref[j, :, columns].T


def transpose_keys(key_cache):
    batch, ctx_dev, width = key_cache.shape
    rows = 2
    return pl.pallas_call(
        transpose_keys_kernel,
        grid=(batch // rows,),
        in_specs=[pl.BlockSpec((rows, ctx_dev, width), lambda s: (s, 0, 0))],
        out_specs=pl.BlockSpec((rows, width, ctx_dev), lambda s: (s, 0, 0)),
        out_shape=hbm_out((batch, width, ctx_dev), key_cache.dtype),
        compiler_params=limit(8),
        interpret=INTERPRET,
        name="transpose_keys",
    )(in_hbm(key_cache))


def attend_kernel(lengths_ref, first_ref, own_ref, partner_ref, key_ref, value_ref,
                  mine_ref, theirs_ref, level_ref, level_theirs_ref, q_scr, o_scr, level_scr,
                  keys_scr, values_scr, sems):
    step = pl.program_id(0)
    blocks = own_ref.shape[0] // NEAR
    batch = mine_ref.shape[1]
    ctx_dev = value_ref.shape[1]
    group = CORES * NEAR
    f32, bf16 = jnp.float32, jnp.bfloat16

    def copies(part):
        rows = pl.ds(part * STEP_ROWS, STEP_ROWS)
        return (
            pltpu.make_async_copy(key_ref.at[rows], keys_scr.at[rows], sems.at[0, part]),
            pltpu.make_async_copy(value_ref.at[rows], values_scr.at[rows], sems.at[1, part]),
        )

    @pl.when(step == 0)
    def _():
        for part in range(batch // STEP_ROWS):
            for copy in copies(part):
                copy.start()
        for g in range(blocks):
            for c, ref in enumerate((own_ref, partner_ref)):
                for i in range(NEAR):
                    row = (g * group + c * NEAR + i) * batch
                    q_scr[row : row + batch, :] = ref[i * blocks + g, :batch, :].astype(f32)
        level_scr[...] = jnp.full(level_scr.shape, EMPTY, f32)

    for copy in copies(step):
        copy.wait()
    lanes = lax.broadcasted_iota(jnp.int32, (group * blocks, ctx_dev), 1)
    level_lanes = lax.broadcasted_iota(jnp.int32, level_scr.shape, 1)
    step_scores = []
    for j in range(STEP_ROWS):
        b = step * STEP_ROWS + j
        scores = []
        for g in range(blocks):
            query = q_scr[pl.ds(g * group * batch + b, group, stride=batch), :].astype(bf16)
            keys = keys_scr[b, g * HEAD_DIM : (g + 1) * HEAD_DIM, :]
            scores.append(jnp.dot(query, keys, preferred_element_type=f32))
        step_scores.append(jnp.concatenate(scores, axis=0) * (1.0 / math.sqrt(HEAD_DIM)))
    step_weights, step_inverse = [], []
    levels = level_scr[...]
    for j in range(STEP_ROWS):
        b = step * STEP_ROWS + j
        used = lanes < lengths_ref[b] - first_ref[0]
        scores = jnp.where(used, step_scores[j], EMPTY)
        top = jnp.max(scores, axis=1, keepdims=True)
        weights = jnp.where(used, jnp.exp(scores - top), 0.0)
        total = jnp.sum(weights, axis=1, keepdims=True)
        some = total > 0
        safe = jnp.where(some, total, 1.0)
        level = jnp.where(some, top + jnp.log(safe), EMPTY)
        levels = jnp.where(level_lanes == b, level, levels)
        step_inverse.append(1.0 / safe)
        step_weights.append(weights.astype(bf16))
    level_scr[...] = levels
    outs = []
    for j in range(STEP_ROWS):
        b = step * STEP_ROWS + j
        for g in range(blocks):
            rows = slice(g * group, (g + 1) * group)
            values = values_scr[b, :, g * HEAD_DIM : (g + 1) * HEAD_DIM]
            out = jnp.dot(step_weights[j][rows], values, preferred_element_type=f32)
            outs.append(out * step_inverse[j][rows])
    for j in range(STEP_ROWS):
        b = step * STEP_ROWS + j
        for g in range(blocks):
            o_scr[pl.ds(g * group * batch + b, group, stride=batch), :] = outs[j * blocks + g]

    @pl.when(step == pl.num_programs(0) - 1)
    def _():
        for g in range(blocks):
            halves = ((mine_ref, level_ref), (theirs_ref, level_theirs_ref))
            for c, (ref, level) in enumerate(halves):
                for i in range(NEAR):
                    row = (g * group + c * NEAR + i) * batch
                    ref[g * NEAR + i] = o_scr[row : row + batch, :].astype(bf16)
                source = g * group + c * NEAR
                level[g * NEAR : (g + 1) * NEAR, :] = level_scr[source : source + NEAR, :]


def attend(lengths, first, own, partner, keys, values):
    batch = keys.shape[0]
    chips = own.shape[0]
    heads = CORES * chips
    return pl.pallas_call(
        attend_kernel,
        grid_spec=pltpu.PrefetchScalarGridSpec(
            num_scalar_prefetch=2,
            grid=(batch // STEP_ROWS,),
            in_specs=[whole(), whole()] + [pl.BlockSpec(memory_space=pl.ANY)] * 2,
            out_specs=[whole()] * 4,
            scratch_shapes=[
                pltpu.VMEM((heads * batch, HEAD_DIM), jnp.float32),
                pltpu.VMEM((heads * batch, HEAD_DIM), jnp.float32),
                pltpu.VMEM((heads, HEAD_DIM), jnp.float32),
                pltpu.VMEM(keys.shape, keys.dtype),
                pltpu.VMEM(values.shape, values.dtype),
                pltpu.SemaphoreType.DMA((2, batch // STEP_ROWS)),
            ],
        ),
        out_shape=[
            vmem_out((chips, batch, HEAD_DIM), jnp.bfloat16),
            vmem_out((chips, batch, HEAD_DIM), jnp.bfloat16),
            vmem_out((chips, HEAD_DIM), jnp.float32),
            vmem_out((chips, HEAD_DIM), jnp.float32),
        ],
        compiler_params=limit(16),
        interpret=INTERPRET,
        name="attend",
    )(lengths, first, in_vmem(own), in_vmem(partner), in_hbm(keys), in_hbm(values))


def sort_columns_kernel(core_ref, w_ref, mine_ref, theirs_ref):
    swap = core_ref[0] == 1
    for i in range(w_ref.shape[1] // (CORES * HEAD_DIM)):
        first = w_ref[:, CORES * i * HEAD_DIM : (CORES * i + 1) * HEAD_DIM]
        second = w_ref[:, (CORES * i + 1) * HEAD_DIM : (CORES * i + 2) * HEAD_DIM]
        columns = slice(i * HEAD_DIM, (i + 1) * HEAD_DIM)
        mine_ref[:, columns] = jnp.where(swap, second, first)
        theirs_ref[:, columns] = jnp.where(swap, first, second)


def sort_columns(core, w_out):
    rows, width = w_out.shape
    steps = 4
    chunk = width // steps
    half = pl.BlockSpec((rows, chunk // CORES), lambda s, *_: (0, s))
    return pl.pallas_call(
        sort_columns_kernel,
        grid_spec=pltpu.PrefetchScalarGridSpec(
            num_scalar_prefetch=1,
            grid=(steps,),
            in_specs=[pl.BlockSpec((rows, chunk), lambda s, *_: (0, s))],
            out_specs=[half, half],
        ),
        out_shape=[jax.ShapeDtypeStruct((rows, width // CORES), w_out.dtype)] * 2,
        compiler_params=limit(8),
        interpret=INTERPRET,
        name="sort_columns",
    )(core, w_out)


def output_kernel(own_ref, partner_ref, w_own_ref, w_partner_ref, out_ref):
    blocks = out_ref.shape[1]
    for z in range(NEAR * blocks):
        columns = slice(z * HEAD_DIM, (z + 1) * HEAD_DIM)
        term = jnp.dot(own_ref[...], w_own_ref[:, columns], preferred_element_type=jnp.float32)
        term += jnp.dot(
            partner_ref[...], w_partner_ref[:, columns], preferred_element_type=jnp.float32
        )
        out_ref[z % NEAR, z // NEAR] = term.astype(out_ref.dtype)


def output_terms(own, partner, w_own, w_partner):
    batch = own.shape[0]
    blocks = w_own.shape[1] // HEAD_DIM // NEAR
    return pl.pallas_call(
        output_kernel,
        in_specs=[whole()] * 4,
        out_specs=whole(),
        out_shape=vmem_out((NEAR, blocks, batch, HEAD_DIM), jnp.bfloat16),
        compiler_params=limit(8),
        interpret=INTERPRET,
        name="output_terms",
    )(in_vmem(own), in_vmem(partner), in_vmem(w_own), in_vmem(w_partner))


def body(hidden_in, w_query, w_keyval, key_cache, value_cache, lengths, w_out):
    batch, ctx_dev, half_width = key_cache.shape
    shards = lax.axis_size("seq")
    index = lax.axis_index("seq")
    core = index % CORES
    chips = shards // CORES
    blocks = chips // NEAR
    heads = w_out.shape[0] // HEAD_DIM * shards
    group = heads // KV_HEADS
    kv_cols = w_keyval.shape[1]
    f32, bf16 = jnp.float32, jnp.bfloat16

    first = (index * ctx_dev).astype(jnp.int32)[None]
    own_group = index // group
    hidden_in, first, core, own_group = lax.optimization_barrier(
        (hidden_in, first, core, own_group)
    )

    packet = project(hidden_in, w_query, w_keyval.T, blocks)
    packet, keys = lax.optimization_barrier((packet, key_cache))
    far = exchange(packet, far_groups(shards))
    keys = transpose_keys(keys)
    far, keys = lax.optimization_barrier((far, keys))
    near = exchange(
        jnp.broadcast_to(far[None], (NEAR, *far.shape)).reshape(chips, *far.shape[1:]),
        near_groups(shards),
    )
    partner = to_partner(near, shards)

    mine, theirs, level, level_theirs = attend(
        lengths, first, near, partner, keys, value_cache
    )

    rows = batch * kv_cols // HEAD_DIM
    kv = jnp.stack([near[:, batch : batch + rows], partner[:, batch : batch + rows]])
    kv = jnp.where(core == 0, kv, kv[::-1]).reshape(CORES, NEAR, blocks, rows, HEAD_DIM)
    kv = kv.transpose(2, 1, 0, 3, 4).reshape(2, KV_HEADS, -1, rows, HEAD_DIM)
    own_kv = lax.dynamic_slice_in_dim(kv, own_group, 1, axis=1)[:, 0]
    own_kv = own_kv.reshape(2, HEAD_DIM // kv_cols, rows, -1, kv_cols).transpose(0, 3, 2, 1, 4)
    own_kv = own_kv.reshape(2, batch, HEAD_DIM).astype(f32)
    query_part = packet[0, :batch].astype(f32)
    score_new = jnp.sum(query_part * own_kv[0], axis=-1) / math.sqrt(HEAD_DIM)

    got_out = to_partner(theirs, shards).astype(f32)
    got_level = to_partner(level_theirs, shards)[:, :batch]
    level = level[:, :batch]
    top = jnp.maximum(level, got_level)
    part_a = jnp.exp(level - top)
    part_b = jnp.exp(got_level - top)
    whole = part_a + part_b
    merged = mine.astype(f32) * (part_a / whole)[..., None] + got_out * (part_b / whole)[..., None]
    level = jnp.maximum(top + jnp.log(whole), EMPTY)
    stats = jnp.concatenate(split_terms(level), axis=1)
    stats = jnp.pad(stats, ((0, 0), (0, HEAD_DIM - stats.shape[1])))
    sent = jnp.concatenate([merged.astype(bf16).reshape(chips, -1), stats], axis=1)
    sent, w_now = lax.optimization_barrier((sent, w_out))
    arrived = exchange(sent[:, None, :], same_core_groups(shards))[:, 0]

    w_mine, w_theirs = sort_columns(core.astype(jnp.int32)[None], w_now)
    w_partner = to_partner(w_theirs, shards)
    q_size = batch * HEAD_DIM
    outs = arrived[:, :q_size].reshape(chips, batch, HEAD_DIM).astype(f32)
    levels = arrived[:, q_size : q_size + 3 * batch].astype(f32).reshape(chips, 3, batch)
    levels = levels[:, 0] + (levels[:, 1] + levels[:, 2])
    top = jnp.maximum(jnp.max(levels, axis=0), score_new)
    factor = jnp.exp(levels - top)
    factor_new = jnp.exp(score_new - top)
    numerator = jnp.sum(outs * factor[..., None], axis=0) + factor_new[:, None] * own_kv[1]
    denominator = jnp.sum(factor, axis=0) + factor_new
    attended = (numerator / denominator[:, None]).astype(bf16)

    attended_partner = to_partner(attended, shards)
    term = output_terms(attended, attended_partner, w_mine, w_partner)
    arrived = exchange(term.reshape(chips, batch, -1), near_groups(shards))
    term = jnp.sum(arrived.reshape(NEAR, blocks, batch, -1).astype(f32), axis=0).astype(bf16)
    arrived = exchange(term, far_groups(shards))
    return jnp.sum(arrived.astype(f32), axis=0).astype(bf16)


def solution(mesh):
    placed = (
        P("replica", None),
        P(None, "seq"),
        P(None, "seq"),
        P("replica", "seq", None),
        P("replica", "seq", None),
        P("replica"),
        P("seq", None),
    )
    return jax.shard_map(
        body, mesh=mesh, in_specs=placed, out_specs=P("replica", "seq"), check_vma=False
    )
```

```python
import functools
import math

import jax
import jax.numpy as jnp
from jax import lax
from jax.experimental import pallas as pl
from jax.experimental.pallas import tpu as pltpu
from jax.sharding import PartitionSpec as P


KV_HEADS = 8
HEAD_DIM = 128
CORES = 2
NEAR = 4
EMPTY = -1e30
PACK_ROWS = 24
STEP_ROWS = 4
INTERPRET = False


def near_groups(shards):
    blocks = shards // CORES // NEAR
    return [
        [CORES * (NEAR * b + i) + c for i in range(NEAR)] for b in range(blocks) for c in range(CORES)
    ]


def far_groups(shards):
    blocks = shards // CORES // NEAR
    return [
        [CORES * (NEAR * b + i) + c for b in range(blocks)] for i in range(NEAR) for c in range(CORES)
    ]


def exchange(x, groups):
    return lax.all_to_all(
        x, "seq", split_axis=0, concat_axis=0, axis_index_groups=groups, tiled=True
    )


def to_partner(x, shards):
    return lax.ppermute(x, "seq", [(i, i ^ 1) for i in range(shards)])


def in_vmem(x):
    return x if INTERPRET else pltpu.with_memory_space_constraint(x, pltpu.VMEM)


def in_hbm(x):
    return x if INTERPRET else pltpu.with_memory_space_constraint(x, pltpu.HBM)


def vmem_out(shape, dtype):
    return jax.ShapeDtypeStruct(shape, dtype) if INTERPRET else pltpu.VMEM(shape, dtype)


def hbm_out(shape, dtype):
    return jax.ShapeDtypeStruct(shape, dtype) if INTERPRET else pltpu.HBM(shape, dtype)


def whole():
    return pl.BlockSpec(memory_space=pltpu.VMEM)


def limit(mib):
    return pltpu.CompilerParams(vmem_limit_bytes=mib << 20)


def project_kernel(hidden_ref, w_query_ref, w_keyval_ref, packet_ref, acc_q, acc_kv):
    step = pl.program_id(0)

    @pl.when(step == 0)
    def _():
        acc_q[...] = jnp.zeros_like(acc_q)
        acc_kv[...] = jnp.zeros_like(acc_kv)

    hidden = hidden_ref[...]
    acc_q[...] += jnp.dot(hidden, w_query_ref[...], preferred_element_type=jnp.float32)
    acc_kv[...] += lax.dot_general(
        hidden, w_keyval_ref[...], (((1,), (1,)), ((), ())), preferred_element_type=jnp.float32
    )

    @pl.when(step == pl.num_programs(0) - 1)
    def _():
        batch, cols = acc_kv.shape
        rows = batch * cols // HEAD_DIM
        keyval = acc_kv[...]
        keyval = jnp.concatenate(
            [keyval[i * rows : (i + 1) * rows] for i in range(HEAD_DIM // cols)], axis=1
        )
        filler = jnp.zeros((PACK_ROWS - batch - rows, HEAD_DIM), jnp.float32)
        packet = jnp.concatenate([acc_q[...], keyval, filler], axis=0).astype(jnp.bfloat16)
        for copy in range(packet_ref.shape[0]):
            packet_ref[copy] = packet


def project(hidden_in, w_query, w_keyval_t, copies):
    batch, width = hidden_in.shape
    cols = w_keyval_t.shape[0]
    steps = 2
    chunk = width // steps
    return pl.pallas_call(
        project_kernel,
        grid=(steps,),
        in_specs=[
            pl.BlockSpec((batch, chunk), lambda k: (0, k)),
            pl.BlockSpec((chunk, HEAD_DIM), lambda k: (k, 0)),
            pl.BlockSpec((cols, chunk), lambda k: (0, k)),
        ],
        out_specs=whole(),
        out_shape=vmem_out((copies, PACK_ROWS, HEAD_DIM), jnp.bfloat16),
        scratch_shapes=[
            pltpu.VMEM((batch, HEAD_DIM), jnp.float32),
            pltpu.VMEM((batch, cols), jnp.float32),
        ],
        compiler_params=limit(8),
        interpret=INTERPRET,
        name="project",
    )(in_hbm(hidden_in), in_hbm(w_query), in_hbm(w_keyval_t))


def transpose_keys_kernel(key_ref, out_ref):
    for j in range(key_ref.shape[0]):
        for g in range(key_ref.shape[2] // HEAD_DIM):
            columns = slice(g * HEAD_DIM, (g + 1) * HEAD_DIM)
            out_ref[j, columns, :] = key_ref[j, :, columns].T


def transpose_keys(key_cache):
    batch, ctx_dev, width = key_cache.shape
    rows = 2
    return pl.pallas_call(
        transpose_keys_kernel,
        grid=(batch // rows,),
        in_specs=[pl.BlockSpec((rows, ctx_dev, width), lambda s: (s, 0, 0))],
        out_specs=pl.BlockSpec((rows, width, ctx_dev), lambda s: (s, 0, 0)),
        out_shape=hbm_out((batch, width, ctx_dev), key_cache.dtype),
        compiler_params=limit(8),
        interpret=INTERPRET,
        name="transpose_keys",
    )(in_hbm(key_cache))


def attend_kernel(lengths_ref, first_ref, own_ref, partner_ref, key_ref, value_ref,
                  mine_ref, theirs_ref, level_ref, level_theirs_ref, q_scr, o_scr, level_scr,
                  keys_scr, values_scr, sems):
    step = pl.program_id(0)
    blocks = own_ref.shape[0] // NEAR
    batch = mine_ref.shape[1]
    ctx_dev = value_ref.shape[1]
    group = CORES * NEAR
    f32, bf16 = jnp.float32, jnp.bfloat16

    def copies(part):
        rows = pl.ds(part * STEP_ROWS, STEP_ROWS)
        return (
            pltpu.make_async_copy(key_ref.at[rows], keys_scr.at[rows], sems.at[0, part]),
            pltpu.make_async_copy(value_ref.at[rows], values_scr.at[rows], sems.at[1, part]),
        )

    @pl.when(step == 0)
    def _():
        for part in range(batch // STEP_ROWS):
            for copy in copies(part):
                copy.start()
        for g in range(blocks):
            for c, ref in enumerate((own_ref, partner_ref)):
                for i in range(NEAR):
                    row = (g * group + c * NEAR + i) * batch
                    q_scr[row : row + batch, :] = ref[i * blocks + g, :batch, :].astype(f32)
        level_scr[...] = jnp.full(level_scr.shape, EMPTY, f32)

    for copy in copies(step):
        copy.wait()
    lanes = lax.broadcasted_iota(jnp.int32, (group * blocks, ctx_dev), 1)
    level_lanes = lax.broadcasted_iota(jnp.int32, level_scr.shape, 1)
    step_scores = []
    for j in range(STEP_ROWS):
        b = step * STEP_ROWS + j
        scores = []
        for g in range(blocks):
            query = q_scr[pl.ds(g * group * batch + b, group, stride=batch), :].astype(bf16)
            keys = keys_scr[b, g * HEAD_DIM : (g + 1) * HEAD_DIM, :]
            scores.append(jnp.dot(query, keys, preferred_element_type=f32))
        step_scores.append(jnp.concatenate(scores, axis=0) * (1.0 / math.sqrt(HEAD_DIM)))
    step_weights, step_inverse = [], []
    levels = level_scr[...]
    for j in range(STEP_ROWS):
        b = step * STEP_ROWS + j
        used = lanes < lengths_ref[b] - first_ref[0]
        scores = jnp.where(used, step_scores[j], EMPTY)
        top = jnp.max(scores, axis=1, keepdims=True)
        weights = jnp.where(used, jnp.exp(scores - top), 0.0)
        total = jnp.sum(weights, axis=1, keepdims=True)
        some = total > 0
        safe = jnp.where(some, total, 1.0)
        level = jnp.where(some, top + jnp.log(safe), EMPTY)
        levels = jnp.where(level_lanes == b, level, levels)
        step_inverse.append(1.0 / safe)
        step_weights.append(weights.astype(bf16))
    level_scr[...] = levels
    outs = []
    for j in range(STEP_ROWS):
        b = step * STEP_ROWS + j
        for g in range(blocks):
            rows = slice(g * group, (g + 1) * group)
            values = values_scr[b, :, g * HEAD_DIM : (g + 1) * HEAD_DIM]
            out = jnp.dot(step_weights[j][rows], values, preferred_element_type=f32)
            outs.append(out * step_inverse[j][rows])
    for j in range(STEP_ROWS):
        b = step * STEP_ROWS + j
        for g in range(blocks):
            o_scr[pl.ds(g * group * batch + b, group, stride=batch), :] = outs[j * blocks + g]

    @pl.when(step == pl.num_programs(0) - 1)
    def _():
        for g in range(blocks):
            for c, ref in enumerate((mine_ref, theirs_ref)):
                for i in range(NEAR):
                    row = (g * group + c * NEAR + i) * batch
                    ref[i * blocks + g] = o_scr[row : row + batch, :].astype(bf16)
        for c, level in enumerate((level_ref, level_theirs_ref)):
            for i in range(NEAR):
                rows = level_scr[pl.ds(c * NEAR + i, blocks, stride=group), :]
                level[i * blocks : (i + 1) * blocks, :] = rows


def attend(lengths, first, own, partner, keys, values):
    batch = keys.shape[0]
    chips = own.shape[0]
    heads = CORES * chips
    return pl.pallas_call(
        attend_kernel,
        grid_spec=pltpu.PrefetchScalarGridSpec(
            num_scalar_prefetch=2,
            grid=(batch // STEP_ROWS,),
            in_specs=[whole(), whole()] + [pl.BlockSpec(memory_space=pl.ANY)] * 2,
            out_specs=[whole()] * 4,
            scratch_shapes=[
                pltpu.VMEM((heads * batch, HEAD_DIM), jnp.float32),
                pltpu.VMEM((heads * batch, HEAD_DIM), jnp.float32),
                pltpu.VMEM((heads, HEAD_DIM), jnp.float32),
                pltpu.VMEM(keys.shape, keys.dtype),
                pltpu.VMEM(values.shape, values.dtype),
                pltpu.SemaphoreType.DMA((2, batch // STEP_ROWS)),
            ],
        ),
        out_shape=[
            vmem_out((chips, batch, HEAD_DIM), jnp.bfloat16),
            vmem_out((chips, batch, HEAD_DIM), jnp.bfloat16),
            vmem_out((chips, HEAD_DIM), jnp.float32),
            vmem_out((chips, HEAD_DIM), jnp.float32),
        ],
        compiler_params=limit(16),
        interpret=INTERPRET,
        name="attend",
    )(lengths, first, in_vmem(own), in_vmem(partner), in_hbm(keys), in_hbm(values))


def as_columns(*parts):
    count = sum(part.shape[0] for part in parts)
    filler = jnp.zeros((HEAD_DIM - count, HEAD_DIM), jnp.float32)
    return jnp.concatenate([*parts, filler], axis=0).T


def write_packet(ref, at, out, level):
    row = lax.broadcasted_iota(jnp.int32, (PACK_ROWS - out.shape[0], HEAD_DIM), 0)
    high = level.astype(jnp.bfloat16).astype(jnp.float32)
    middle = (level - high).astype(jnp.bfloat16).astype(jnp.float32)
    low = level - high - middle
    stats = jnp.where(row == 0, high, jnp.where(row == 1, middle, jnp.where(row == 2, low, 0.0)))
    ref[at] = jnp.concatenate([out, stats], axis=0).astype(jnp.bfloat16)


def read_levels(ref, batch, scr):
    for r in range(ref.shape[0]):
        stats = ref[r, batch:, :].astype(jnp.float32)
        scr[r : r + 1, :] = stats[0:1] + (stats[1:2] + stats[2:3])
    return scr[...]


def merge_cores_kernel(mine_ref, level_ref, got_ref, got_level_ref, out_ref):
    batch = mine_ref.shape[1]
    count = mine_ref.shape[0]
    level, got = level_ref[...], got_level_ref[...]
    top = jnp.maximum(level, got)
    part_a, part_b = jnp.exp(level - top), jnp.exp(got - top)
    total = part_a + part_b
    merged = top + jnp.log(total)
    columns = as_columns(part_a / total, part_b / total)
    for r in range(count):
        out = mine_ref[r].astype(jnp.float32) * columns[:batch, r : r + 1]
        out += got_ref[r].astype(jnp.float32) * columns[:batch, count + r : count + r + 1]
        write_packet(out_ref, r, out, merged[r : r + 1, :])


def merge_cores(mine, level, got, got_level):
    chips, _, _ = mine.shape
    return pl.pallas_call(
        merge_cores_kernel,
        in_specs=[whole()] * 4,
        out_specs=whole(),
        out_shape=vmem_out((chips, PACK_ROWS, HEAD_DIM), jnp.bfloat16),
        compiler_params=limit(8),
        interpret=INTERPRET,
        name="merge_cores",
    )(in_vmem(mine), in_vmem(level), in_vmem(got), in_vmem(got_level))


def merge_near_kernel(batch, packet_ref, out_ref, level_scr):
    blocks = out_ref.shape[0]
    levels = read_levels(packet_ref, batch, level_scr)
    parts = [levels[i * blocks : (i + 1) * blocks] for i in range(NEAR)]
    top = functools.reduce(jnp.maximum, parts)
    parts = [jnp.exp(part - top) for part in parts]
    total = functools.reduce(jnp.add, parts)
    merged = top + jnp.log(total)
    columns = as_columns(*[part / total for part in parts])
    for k in range(blocks):
        out = 0.0
        for i in range(NEAR):
            r = i * blocks + k
            rows = packet_ref[r, :batch, :].astype(jnp.float32)
            out += rows * columns[:batch, r : r + 1]
        write_packet(out_ref, k, out, merged[k : k + 1, :])


def merge_near(packets, batch):
    count = packets.shape[0]
    return pl.pallas_call(
        functools.partial(merge_near_kernel, batch),
        in_specs=[whole()],
        out_specs=whole(),
        out_shape=vmem_out((count // NEAR, PACK_ROWS, HEAD_DIM), jnp.bfloat16),
        scratch_shapes=[pltpu.VMEM((count, HEAD_DIM), jnp.float32)],
        compiler_params=limit(8),
        interpret=INTERPRET,
        name="merge_near",
    )(in_vmem(packets))


def merge_far_kernel(packet_ref, score_ref, value_ref, out_ref, level_scr):
    batch = out_ref.shape[0]
    count = packet_ref.shape[0]
    levels = read_levels(packet_ref, batch, level_scr)
    score = score_ref[...]
    top = jnp.maximum(jnp.max(levels, axis=0, keepdims=True), score)
    parts, part_new = jnp.exp(levels - top), jnp.exp(score - top)
    total = jnp.sum(parts, axis=0, keepdims=True) + part_new
    columns = as_columns(parts / total, part_new / total)
    out = value_ref[...] * columns[:batch, count : count + 1]
    for r in range(count):
        out += packet_ref[r, :batch, :].astype(jnp.float32) * columns[:batch, r : r + 1]
    out_ref[...] = out.astype(out_ref.dtype)


def merge_far(packets, score_new, value_new):
    count = packets.shape[0]
    batch = value_new.shape[0]
    return pl.pallas_call(
        merge_far_kernel,
        in_specs=[whole()] * 3,
        out_specs=whole(),
        out_shape=vmem_out((batch, HEAD_DIM), jnp.bfloat16),
        scratch_shapes=[pltpu.VMEM((count, HEAD_DIM), jnp.float32)],
        compiler_params=limit(8),
        interpret=INTERPRET,
        name="merge_far",
    )(in_vmem(packets), in_vmem(score_new), in_vmem(value_new))


def new_token_kernel(where_ref, query_ref, own_ref, partner_ref, score_ref, value_ref):
    core, own_group = where_ref[0], where_ref[1]
    batch = value_ref.shape[0]
    blocks = own_ref.shape[0] // NEAR
    group_chips = own_ref.shape[0] // (2 * KV_HEADS)
    rows_of = []
    for half in range(2):
        pieces = []
        for e in range(group_chips):
            chip = (half * KV_HEADS + own_group) * group_chips + e
            at = chip % NEAR * blocks + chip // NEAR
            own = own_ref[at, batch:, :].astype(jnp.float32)
            partner = partner_ref[at, batch:, :].astype(jnp.float32)
            pieces += [jnp.where(core == 0, own, partner), jnp.where(core == 0, partner, own)]
        cols = HEAD_DIM // len(pieces)
        rows = batch * cols // HEAD_DIM
        parts = []
        for q in range(HEAD_DIM // cols):
            lanes = slice(q * cols, (q + 1) * cols)
            parts.append(jnp.concatenate([piece[:rows, lanes] for piece in pieces], axis=1))
        rows_of.append(jnp.concatenate(parts, axis=0))
    query = query_ref[0, :batch, :].astype(jnp.float32)
    score = jnp.sum(query * rows_of[0], axis=1, keepdims=True) * (1.0 / math.sqrt(HEAD_DIM))
    row = lax.broadcasted_iota(jnp.int32, (batch, HEAD_DIM), 0)
    lane = lax.broadcasted_iota(jnp.int32, (batch, HEAD_DIM), 1)
    score_ref[...] = jnp.sum(jnp.where(row == lane, score, 0.0), axis=0, keepdims=True)
    value_ref[...] = rows_of[1]


def new_token(where, packet, own, partner, batch):
    return pl.pallas_call(
        new_token_kernel,
        grid_spec=pltpu.PrefetchScalarGridSpec(
            num_scalar_prefetch=1,
            grid=(1,),
            in_specs=[whole()] * 3,
            out_specs=[whole()] * 2,
        ),
        out_shape=[
            vmem_out((1, HEAD_DIM), jnp.float32),
            vmem_out((batch, HEAD_DIM), jnp.float32),
        ],
        compiler_params=limit(8),
        interpret=INTERPRET,
        name="new_token",
    )(where, in_vmem(packet), in_vmem(own), in_vmem(partner))


def sort_columns_kernel(core_ref, w_ref, mine_ref, theirs_ref):
    swap = core_ref[0] == 1
    for i in range(w_ref.shape[1] // (CORES * HEAD_DIM)):
        first = w_ref[:, CORES * i * HEAD_DIM : (CORES * i + 1) * HEAD_DIM]
        second = w_ref[:, (CORES * i + 1) * HEAD_DIM : (CORES * i + 2) * HEAD_DIM]
        columns = slice(i * HEAD_DIM, (i + 1) * HEAD_DIM)
        mine_ref[:, columns] = jnp.where(swap, second, first)
        theirs_ref[:, columns] = jnp.where(swap, first, second)


def sort_columns(core, w_out):
    rows, width = w_out.shape
    steps = 4
    chunk = width // steps
    half = pl.BlockSpec((rows, chunk // CORES), lambda s, *_: (0, s))
    return pl.pallas_call(
        sort_columns_kernel,
        grid_spec=pltpu.PrefetchScalarGridSpec(
            num_scalar_prefetch=1,
            grid=(steps,),
            in_specs=[pl.BlockSpec((rows, chunk), lambda s, *_: (0, s))],
            out_specs=[half, half],
        ),
        out_shape=[jax.ShapeDtypeStruct((rows, width // CORES), w_out.dtype)] * 2,
        compiler_params=limit(8),
        interpret=INTERPRET,
        name="sort_columns",
    )(core, w_out)


def output_kernel(own_ref, partner_ref, w_own_ref, w_partner_ref, out_ref):
    blocks = out_ref.shape[1]
    for z in range(NEAR * blocks):
        columns = slice(z * HEAD_DIM, (z + 1) * HEAD_DIM)
        term = jnp.dot(own_ref[...], w_own_ref[:, columns], preferred_element_type=jnp.float32)
        term += jnp.dot(
            partner_ref[...], w_partner_ref[:, columns], preferred_element_type=jnp.float32
        )
        out_ref[z % NEAR, z // NEAR] = term.astype(out_ref.dtype)


def output_terms(own, partner, w_own, w_partner):
    batch = own.shape[0]
    blocks = w_own.shape[1] // HEAD_DIM // NEAR
    return pl.pallas_call(
        output_kernel,
        in_specs=[whole()] * 4,
        out_specs=whole(),
        out_shape=vmem_out((NEAR, blocks, batch, HEAD_DIM), jnp.bfloat16),
        compiler_params=limit(8),
        interpret=INTERPRET,
        name="output_terms",
    )(in_vmem(own), in_vmem(partner), in_vmem(w_own), in_vmem(w_partner))


def layer(hidden_in, w_query, w_keyval, key_cache, value_cache, lengths, w_out):
    batch, ctx_dev, _ = key_cache.shape
    shards = lax.axis_size("seq")
    index = lax.axis_index("seq")
    core = index % CORES
    chips = shards // CORES
    blocks = chips // NEAR
    heads = w_out.shape[0] // HEAD_DIM * shards
    group = heads // KV_HEADS
    f32, bf16 = jnp.float32, jnp.bfloat16

    first = (index * ctx_dev).astype(jnp.int32)[None]
    where = jnp.stack([core, index // group]).astype(jnp.int32)
    hidden_in, first, where = lax.optimization_barrier((hidden_in, first, where))

    packet = project(hidden_in, w_query, w_keyval.T, blocks)
    packet, keys = lax.optimization_barrier((packet, key_cache))
    far = exchange(packet, far_groups(shards))
    keys = transpose_keys(keys)
    far, keys = lax.optimization_barrier((far, keys))
    near = exchange(
        jnp.broadcast_to(far[None], (NEAR, *far.shape)).reshape(chips, *far.shape[1:]),
        near_groups(shards),
    )
    partner = to_partner(near, shards)

    mine, theirs, level, level_theirs = attend(
        lengths, first, near, partner, keys, value_cache
    )

    got = to_partner(theirs, shards)
    got_level = to_partner(level_theirs, shards)
    packets = exchange(merge_cores(mine, level, got, got_level), near_groups(shards))
    packets = merge_near(packets, batch)
    packets = exchange(packets, far_groups(shards))

    score_new, value_new = new_token(where, packet, near, partner, batch)
    w_mine, w_theirs = sort_columns(where, w_out)
    w_partner = to_partner(w_theirs, shards)
    attended = merge_far(packets, score_new, value_new)

    attended_partner = to_partner(attended, shards)
    term = output_terms(attended, attended_partner, w_mine, w_partner)
    arrived = exchange(term.reshape(chips, batch, -1), near_groups(shards))
    term = jnp.sum(arrived.reshape(NEAR, blocks, batch, -1).astype(f32), axis=0).astype(bf16)
    arrived = exchange(term, far_groups(shards))
    return jnp.sum(arrived.astype(f32), axis=0).astype(bf16)


def solution(mesh):
    placed = (
        P("replica", None),
        P(None, "seq"),
        P(None, "seq"),
        P("replica", "seq", None),
        P("replica", "seq", None),
        P("replica"),
        P("seq", None),
    )
    return jax.shard_map(
        layer, mesh=mesh, in_specs=placed, out_specs=P("replica", "seq"), check_vma=False
    )
```

```python
import functools
import math

import jax
import jax.numpy as jnp
from jax import lax
from jax.experimental import pallas as pl
from jax.experimental.pallas import tpu as pltpu
from jax.sharding import PartitionSpec as P


KV_HEADS = 8
HEAD_DIM = 128
CORES = 2
NEAR = 4
EMPTY = -1e30
PACK_ROWS = 24
STEP_ROWS = 4
INTERPRET = False


def near_groups(shards):
    blocks = shards // CORES // NEAR
    return [
        [CORES * (NEAR * b + i) + c for i in range(NEAR)] for b in range(blocks) for c in range(CORES)
    ]


def far_groups(shards):
    blocks = shards // CORES // NEAR
    return [
        [CORES * (NEAR * b + i) + c for b in range(blocks)] for i in range(NEAR) for c in range(CORES)
    ]


def exchange(x, groups):
    return lax.all_to_all(
        x, "seq", split_axis=0, concat_axis=0, axis_index_groups=groups, tiled=True
    )


def to_partner(x, shards):
    return lax.ppermute(x, "seq", [(i, i ^ 1) for i in range(shards)])


def in_vmem(x):
    return x if INTERPRET else pltpu.with_memory_space_constraint(x, pltpu.VMEM)


def in_hbm(x):
    return x if INTERPRET else pltpu.with_memory_space_constraint(x, pltpu.HBM)


def vmem_out(shape, dtype):
    return jax.ShapeDtypeStruct(shape, dtype) if INTERPRET else pltpu.VMEM(shape, dtype)


def hbm_out(shape, dtype):
    return jax.ShapeDtypeStruct(shape, dtype) if INTERPRET else pltpu.HBM(shape, dtype)


def whole():
    return pl.BlockSpec(memory_space=pltpu.VMEM)


def limit(mib):
    return pltpu.CompilerParams(vmem_limit_bytes=mib << 20)


def project_kernel(hidden_ref, w_query_ref, w_keyval_ref, packet_ref, acc_q, acc_kv):
    step = pl.program_id(0)

    @pl.when(step == 0)
    def _():
        acc_q[...] = jnp.zeros_like(acc_q)
        acc_kv[...] = jnp.zeros_like(acc_kv)

    hidden = hidden_ref[...]
    acc_q[...] += jnp.dot(hidden, w_query_ref[...], preferred_element_type=jnp.float32)
    acc_kv[...] += lax.dot_general(
        hidden, w_keyval_ref[...], (((1,), (1,)), ((), ())), preferred_element_type=jnp.float32
    )

    @pl.when(step == pl.num_programs(0) - 1)
    def _():
        batch, cols = acc_kv.shape
        rows = batch * cols // HEAD_DIM
        keyval = acc_kv[...]
        keyval = jnp.concatenate(
            [keyval[i * rows : (i + 1) * rows] for i in range(HEAD_DIM // cols)], axis=1
        )
        filler = jnp.zeros((PACK_ROWS - batch - rows, HEAD_DIM), jnp.float32)
        packet = jnp.concatenate([acc_q[...], keyval, filler], axis=0).astype(jnp.bfloat16)
        for copy in range(packet_ref.shape[0]):
            packet_ref[copy] = packet


def project(hidden_in, w_query, w_keyval_t, copies):
    batch, width = hidden_in.shape
    cols = w_keyval_t.shape[0]
    steps = 2
    chunk = width // steps
    return pl.pallas_call(
        project_kernel,
        grid=(steps,),
        in_specs=[
            pl.BlockSpec((batch, chunk), lambda k: (0, k)),
            pl.BlockSpec((chunk, HEAD_DIM), lambda k: (k, 0)),
            pl.BlockSpec((cols, chunk), lambda k: (0, k)),
        ],
        out_specs=whole(),
        out_shape=vmem_out((copies, PACK_ROWS, HEAD_DIM), jnp.bfloat16),
        scratch_shapes=[
            pltpu.VMEM((batch, HEAD_DIM), jnp.float32),
            pltpu.VMEM((batch, cols), jnp.float32),
        ],
        compiler_params=limit(8),
        interpret=INTERPRET,
        name="project",
    )(in_hbm(hidden_in), in_hbm(w_query), in_hbm(w_keyval_t))


def new_token(where_ref, own_ref, partner_ref, score_ref, value_ref):
    core, own_group, own_at = where_ref[0], where_ref[1], where_ref[2]
    batch = value_ref.shape[0]
    blocks = own_ref.shape[0] // NEAR
    group_chips = own_ref.shape[0] // (2 * KV_HEADS)
    halves = []
    for half in range(2):
        pieces = []
        for e in range(group_chips):
            chip = (half * KV_HEADS + own_group) * group_chips + e
            at = chip % NEAR * blocks + chip // NEAR
            own = own_ref[at, batch:, :].astype(jnp.float32)
            partner = partner_ref[at, batch:, :].astype(jnp.float32)
            pieces += [jnp.where(core == 0, own, partner), jnp.where(core == 0, partner, own)]
        cols = HEAD_DIM // len(pieces)
        rows = batch * cols // HEAD_DIM
        parts = []
        for q in range(HEAD_DIM // cols):
            lanes = slice(q * cols, (q + 1) * cols)
            parts.append(jnp.concatenate([piece[:rows, lanes] for piece in pieces], axis=1))
        halves.append(jnp.concatenate(parts, axis=0))
    query = own_ref[own_at, :batch, :].astype(jnp.float32)
    score = jnp.sum(query * halves[0], axis=1, keepdims=True) * (1.0 / math.sqrt(HEAD_DIM))
    row = lax.broadcasted_iota(jnp.int32, (batch, HEAD_DIM), 0)
    lane = lax.broadcasted_iota(jnp.int32, (batch, HEAD_DIM), 1)
    score_ref[...] = jnp.sum(jnp.where(row == lane, score, 0.0), axis=0, keepdims=True)
    value_ref[...] = halves[1]


def attend_kernel(where_ref, cached_ref, own_ref, partner_ref, key_ref, value_ref,
                  mine_ref, theirs_ref, level_ref, level_theirs_ref, score_ref, new_value_ref,
                  q_scr, s_scr, o_scr, level_scr, keys_scr, values_scr, sems):
    blocks = own_ref.shape[0] // NEAR
    batch, ctx_dev, _ = key_ref.shape
    group = CORES * NEAR
    pack = group * batch
    parts = batch // STEP_ROWS
    f32, bf16 = jnp.float32, jnp.bfloat16

    def copy_of(kind, part):
        rows = pl.ds(part * STEP_ROWS, STEP_ROWS)
        source, target = ((key_ref, keys_scr), (value_ref, values_scr))[kind]
        return pltpu.make_async_copy(source.at[rows], target.at[rows], sems.at[kind, part])

    for kind in range(2):
        for part in range(parts):
            copy_of(kind, part).start()

    for g in range(blocks):
        for c, ref in enumerate((own_ref, partner_ref)):
            for i in range(NEAR):
                start = g * pack + c * NEAR + i
                tile = ref[i * blocks + g, :batch, :].astype(f32)
                q_scr[pl.ds(start, batch, stride=group), :] = tile
    for g in range(blocks):
        rows = slice(g * pack, (g + 1) * pack)
        q_scr[rows, :] = q_scr[rows, :].T
    new_token(where_ref, own_ref, partner_ref, score_ref, new_value_ref)

    lane_row = lax.broadcasted_iota(jnp.int32, (HEAD_DIM, pack), 1) // group
    s_scr[...] = jnp.zeros_like(s_scr)

    def score_part(part, carry):
        copy_of(0, part).wait()
        for g in range(blocks):
            columns = slice(g * HEAD_DIM, (g + 1) * HEAD_DIM)
            query = q_scr[g * pack : (g + 1) * pack, :]
            total = s_scr[g]
            for j in range(0, STEP_ROWS, 2):
                b = part * STEP_ROWS + j
                keys = jnp.concatenate(
                    [keys_scr[b, :, columns], keys_scr[b + 1, :, columns]], axis=1
                )
                picked = jnp.concatenate(
                    [
                        jnp.where(lane_row == b, query, 0.0).astype(bf16),
                        jnp.where(lane_row == b + 1, query, 0.0).astype(bf16),
                    ],
                    axis=0,
                )
                total += jnp.dot(keys, picked, preferred_element_type=f32)
            s_scr[g] = total
        return carry

    lax.fori_loop(0, parts, score_part, 0)

    level_scr[...] = jnp.full(level_scr.shape, EMPTY, f32)
    slot = lax.broadcasted_iota(jnp.int32, (ctx_dev, pack), 0)
    used = slot < cached_ref[...]
    for g in range(blocks):
        scores = jnp.where(used, s_scr[g] * (1.0 / math.sqrt(HEAD_DIM)), EMPTY)
        top = jnp.max(scores, axis=0, keepdims=True)
        weights = jnp.where(used, jnp.exp(scores - top), 0.0)
        total = jnp.sum(weights, axis=0, keepdims=True)
        some = total > 0
        safe = jnp.where(some, total, 1.0)
        level_scr[g : g + 1, :] = jnp.where(some, top + jnp.log(safe), EMPTY)
        s_scr[g] = (weights / safe).T

    def value_part(part, carry):
        copy_of(1, part).wait()
        for j in range(STEP_ROWS):
            b = part * STEP_ROWS + j
            start = pl.multiple_of(b * group, group)
            for g in range(blocks):
                weights = s_scr[g, pl.ds(start, group), :].astype(bf16)
                values = values_scr[b, :, g * HEAD_DIM : (g + 1) * HEAD_DIM]
                out = jnp.dot(weights, values, preferred_element_type=f32)
                o_scr[pl.ds(g * pack + start, group), :] = out
        return carry

    lax.fori_loop(0, parts, value_part, 0)

    level_scr[...] = level_scr[...].T
    for c, (ref, level) in enumerate(((mine_ref, level_ref), (theirs_ref, level_theirs_ref))):
        for i in range(NEAR):
            at = c * NEAR + i
            rows = slice(i * batch, (i + 1) * batch)
            level[rows, :] = level_scr[pl.ds(at, batch, stride=group), :]
            for g in range(blocks):
                tile = o_scr[pl.ds(g * pack + at, batch, stride=group), :]
                ref[i * blocks + g] = tile.astype(bf16)


def attend(where, cached, own, partner, keys, values):
    batch, ctx_dev, _ = keys.shape
    chips = own.shape[0]
    blocks = chips // NEAR
    pack = CORES * NEAR * batch
    f32, bf16 = jnp.float32, jnp.bfloat16
    return pl.pallas_call(
        attend_kernel,
        grid_spec=pltpu.PrefetchScalarGridSpec(
            num_scalar_prefetch=1,
            grid=(1,),
            in_specs=[whole()] * 3 + [pl.BlockSpec(memory_space=pl.ANY)] * 2,
            out_specs=[whole()] * 6,
            scratch_shapes=[
                pltpu.VMEM((blocks * pack, HEAD_DIM), f32),
                pltpu.VMEM((blocks, ctx_dev, pack), f32),
                pltpu.VMEM((blocks * pack, HEAD_DIM), f32),
                pltpu.VMEM((pack, HEAD_DIM), f32),
                pltpu.VMEM(keys.shape, keys.dtype),
                pltpu.VMEM(values.shape, values.dtype),
                pltpu.SemaphoreType.DMA((2, batch // STEP_ROWS)),
            ],
        ),
        out_shape=[
            vmem_out((chips, batch, HEAD_DIM), bf16),
            vmem_out((chips, batch, HEAD_DIM), bf16),
            vmem_out((NEAR * batch, HEAD_DIM), f32),
            vmem_out((NEAR * batch, HEAD_DIM), f32),
            vmem_out((1, HEAD_DIM), f32),
            vmem_out((batch, HEAD_DIM), f32),
        ],
        compiler_params=limit(24),
        interpret=INTERPRET,
        name="attend",
    )(where, in_vmem(cached), in_vmem(own), in_vmem(partner), in_hbm(keys), in_hbm(values))


def as_columns(*parts):
    count = sum(part.shape[0] for part in parts)
    filler = jnp.zeros((HEAD_DIM - count, HEAD_DIM), jnp.float32)
    return jnp.concatenate([*parts, filler], axis=0).T


def write_packet(ref, at, out, level):
    row = lax.broadcasted_iota(jnp.int32, (PACK_ROWS - out.shape[0], HEAD_DIM), 0)
    high = level.astype(jnp.bfloat16).astype(jnp.float32)
    middle = (level - high).astype(jnp.bfloat16).astype(jnp.float32)
    low = level - high - middle
    stats = jnp.where(row == 0, high, jnp.where(row == 1, middle, jnp.where(row == 2, low, 0.0)))
    ref[at] = jnp.concatenate([out, stats], axis=0).astype(jnp.bfloat16)


def read_levels(ref, batch, scr):
    for r in range(ref.shape[0]):
        stats = ref[r, batch:, :].astype(jnp.float32)
        scr[r : r + 1, :] = stats[0:1] + (stats[1:2] + stats[2:3])
    return scr[...]


def merge_cores_kernel(mine_ref, level_ref, got_ref, got_level_ref, out_ref):
    count, batch, _ = mine_ref.shape
    blocks = count // NEAR
    level, got = level_ref[...], got_level_ref[...]
    top = jnp.maximum(level, got)
    part_a, part_b = jnp.exp(level - top), jnp.exp(got - top)
    total = part_a + part_b
    part_a, part_b = part_a / total, part_b / total
    merged = as_columns(top + jnp.log(total))[:blocks]
    for i in range(NEAR):
        rows = slice(i * batch, (i + 1) * batch)
        levels = pltpu.roll(merged, (HEAD_DIM - i * batch) % HEAD_DIM, 1) if i else merged
        for k in range(blocks):
            r = i * blocks + k
            out = mine_ref[r].astype(jnp.float32) * part_a[rows, k : k + 1]
            out += got_ref[r].astype(jnp.float32) * part_b[rows, k : k + 1]
            write_packet(out_ref, r, out, levels[k : k + 1, :])


def merge_cores(mine, level, got, got_level):
    chips, batch, _ = mine.shape
    return pl.pallas_call(
        merge_cores_kernel,
        in_specs=[whole()] * 4,
        out_specs=whole(),
        out_shape=vmem_out((chips, PACK_ROWS, HEAD_DIM), jnp.bfloat16),
        compiler_params=limit(8),
        interpret=INTERPRET,
        name="merge_cores",
    )(in_vmem(mine), in_vmem(level), in_vmem(got), in_vmem(got_level))


def merge_near_kernel(batch, packet_ref, out_ref, level_scr):
    blocks = out_ref.shape[0]
    levels = read_levels(packet_ref, batch, level_scr)
    parts = [levels[i * blocks : (i + 1) * blocks] for i in range(NEAR)]
    top = functools.reduce(jnp.maximum, parts)
    parts = [jnp.exp(part - top) for part in parts]
    total = functools.reduce(jnp.add, parts)
    merged = top + jnp.log(total)
    columns = as_columns(*[part / total for part in parts])
    for k in range(blocks):
        out = 0.0
        for i in range(NEAR):
            r = i * blocks + k
            rows = packet_ref[r, :batch, :].astype(jnp.float32)
            out += rows * columns[:batch, r : r + 1]
        write_packet(out_ref, k, out, merged[k : k + 1, :])


def merge_near(packets, batch):
    count = packets.shape[0]
    return pl.pallas_call(
        functools.partial(merge_near_kernel, batch),
        in_specs=[whole()],
        out_specs=whole(),
        out_shape=vmem_out((count // NEAR, PACK_ROWS, HEAD_DIM), jnp.bfloat16),
        scratch_shapes=[pltpu.VMEM((count, HEAD_DIM), jnp.float32)],
        compiler_params=limit(8),
        interpret=INTERPRET,
        name="merge_near",
    )(in_vmem(packets))


def merge_far_kernel(packet_ref, score_ref, value_ref, out_ref, level_scr):
    batch = out_ref.shape[0]
    count = packet_ref.shape[0]
    levels = read_levels(packet_ref, batch, level_scr)
    score = score_ref[...]
    top = jnp.maximum(jnp.max(levels, axis=0, keepdims=True), score)
    parts, part_new = jnp.exp(levels - top), jnp.exp(score - top)
    total = jnp.sum(parts, axis=0, keepdims=True) + part_new
    columns = as_columns(parts / total, part_new / total)
    out = value_ref[...] * columns[:batch, count : count + 1]
    for r in range(count):
        out += packet_ref[r, :batch, :].astype(jnp.float32) * columns[:batch, r : r + 1]
    out_ref[...] = out.astype(out_ref.dtype)


def merge_far(packets, score_new, value_new):
    count = packets.shape[0]
    batch = value_new.shape[0]
    return pl.pallas_call(
        merge_far_kernel,
        in_specs=[whole()] * 3,
        out_specs=whole(),
        out_shape=vmem_out((batch, HEAD_DIM), jnp.bfloat16),
        scratch_shapes=[pltpu.VMEM((count, HEAD_DIM), jnp.float32)],
        compiler_params=limit(8),
        interpret=INTERPRET,
        name="merge_far",
    )(in_vmem(packets), in_vmem(score_new), in_vmem(value_new))


def output_kernel(where_ref, attended_ref, w_ref, mine_ref, theirs_ref):
    swap = where_ref[0] == 1
    attended = attended_ref[...]
    for i in range(NEAR):
        start = CORES * i * HEAD_DIM
        term = jnp.dot(
            attended,
            w_ref[:, start : start + CORES * HEAD_DIM],
            preferred_element_type=jnp.float32,
        )
        first, second = term[:, :HEAD_DIM], term[:, HEAD_DIM:]
        mine_ref[i, 0] = jnp.where(swap, second, first).astype(mine_ref.dtype)
        theirs_ref[i, 0] = jnp.where(swap, first, second).astype(theirs_ref.dtype)


def output_terms(where, attended, w_out):
    batch = attended.shape[0]
    rows, width = w_out.shape
    chunk = NEAR * CORES * HEAD_DIM
    blocks = width // chunk
    half = pl.BlockSpec((NEAR, 1, batch, HEAD_DIM), lambda s, *_: (0, s, 0, 0))
    return pl.pallas_call(
        output_kernel,
        grid_spec=pltpu.PrefetchScalarGridSpec(
            num_scalar_prefetch=1,
            grid=(blocks,),
            in_specs=[whole(), pl.BlockSpec((rows, chunk), lambda s, *_: (0, s))],
            out_specs=[half, half],
        ),
        out_shape=[vmem_out((NEAR, blocks, batch, HEAD_DIM), jnp.bfloat16)] * 2,
        compiler_params=limit(8),
        interpret=INTERPRET,
        name="output_terms",
    )(where, in_vmem(attended), w_out)


def body(hidden_in, w_query, w_keyval, key_cache, value_cache, lengths, w_out):
    batch, ctx_dev, half_width = key_cache.shape
    shards = lax.axis_size("seq")
    index = lax.axis_index("seq")
    core = index % CORES
    chips = shards // CORES
    blocks = chips // NEAR
    heads = w_out.shape[0] // HEAD_DIM * shards
    group = heads // KV_HEADS
    f32, bf16 = jnp.float32, jnp.bfloat16

    chip = index // CORES
    own_at = chip % NEAR * blocks + chip // NEAR
    where = jnp.stack([core, index // group, own_at]).astype(jnp.int32)
    cached = jnp.repeat(lengths - index * ctx_dev, group)[None]
    hidden_in, where, cached = lax.optimization_barrier((hidden_in, where, cached))

    packet = project(hidden_in, w_query, w_keyval.T, blocks)
    far = exchange(packet, far_groups(shards))
    near = exchange(
        jnp.broadcast_to(far[None], (NEAR, *far.shape)).reshape(chips, *far.shape[1:]),
        near_groups(shards),
    )
    partner = to_partner(near, shards)

    mine, theirs, level, level_theirs, score_new, value_new = attend(
        where, cached, near, partner, key_cache, value_cache
    )

    got = to_partner(theirs, shards)
    got_level = to_partner(level_theirs, shards)
    packets = exchange(merge_cores(mine, level, got, got_level), near_groups(shards))
    packets = exchange(merge_near(packets, batch), far_groups(shards))
    attended = merge_far(packets, score_new, value_new)

    mine, theirs = output_terms(where, attended, w_out)
    term = (mine.astype(f32) + to_partner(theirs, shards).astype(f32)).astype(bf16)
    arrived = exchange(term.reshape(chips, batch, -1), near_groups(shards))
    term = jnp.sum(arrived.reshape(NEAR, blocks, batch, -1).astype(f32), axis=0).astype(bf16)
    arrived = exchange(term, far_groups(shards))
    return jnp.sum(arrived.astype(f32), axis=0).astype(bf16)


def solution(mesh):
    placed = (
        P("replica", None),
        P(None, "seq"),
        P(None, "seq"),
        P("replica", "seq", None),
        P("replica", "seq", None),
        P("replica"),
        P("seq", None),
    )
    step = jax.shard_map(
        body, mesh=mesh, in_specs=placed, out_specs=P("replica", "seq"), check_vma=False
    )
    return step
```

```python
import functools
import math

import jax
import jax.numpy as jnp
from jax import lax
from jax.experimental import pallas as pl
from jax.experimental.pallas import tpu as pltpu
from jax.sharding import PartitionSpec as P


KV_HEADS = 8
HEAD_DIM = 128
CORES = 2
NEAR = 4
EMPTY = -1e30
FIRST_EIGHTH = 6
PACK_ROWS = 24
STEP_ROWS = 4
INTERPRET = False


def near_groups(shards):
    blocks = shards // CORES // NEAR
    return [
        [CORES * (NEAR * b + i) + c for i in range(NEAR)] for b in range(blocks) for c in range(CORES)
    ]


def block_order(blocks):
    return [(p + blocks * FIRST_EIGHTH // 8) % blocks for p in range(blocks)]


def place_of(block, blocks):
    return (block + blocks - blocks * FIRST_EIGHTH // 8) % blocks


def far_groups(shards):
    order = block_order(shards // CORES // NEAR)
    return [
        [CORES * (NEAR * b + i) + c for b in order] for i in range(NEAR) for c in range(CORES)
    ]


def exchange(x, groups):
    return lax.all_to_all(
        x, "seq", split_axis=0, concat_axis=0, axis_index_groups=groups, tiled=True
    )


def to_partner(x, shards):
    return lax.ppermute(x, "seq", [(i, i ^ 1) for i in range(shards)])


def in_vmem(x):
    return x if INTERPRET else pltpu.with_memory_space_constraint(x, pltpu.VMEM)


def in_hbm(x):
    return x if INTERPRET else pltpu.with_memory_space_constraint(x, pltpu.HBM)


def vmem_out(shape, dtype):
    return jax.ShapeDtypeStruct(shape, dtype) if INTERPRET else pltpu.VMEM(shape, dtype)


def hbm_out(shape, dtype):
    return jax.ShapeDtypeStruct(shape, dtype) if INTERPRET else pltpu.HBM(shape, dtype)


def whole():
    return pl.BlockSpec(memory_space=pltpu.VMEM)


def limit(mib):
    return pltpu.CompilerParams(vmem_limit_bytes=mib << 20)


def project_kernel(hidden_ref, w_query_ref, w_keyval_ref, packet_ref, acc_q, acc_kv):
    step = pl.program_id(0)

    @pl.when(step == 0)
    def _():
        acc_q[...] = jnp.zeros_like(acc_q)
        acc_kv[...] = jnp.zeros_like(acc_kv)

    hidden = hidden_ref[...]
    acc_q[...] += jnp.dot(hidden, w_query_ref[...], preferred_element_type=jnp.float32)
    acc_kv[...] += lax.dot_general(
        hidden, w_keyval_ref[...], (((1,), (1,)), ((), ())), preferred_element_type=jnp.float32
    )

    @pl.when(step == pl.num_programs(0) - 1)
    def _():
        batch, cols = acc_kv.shape
        rows = batch * cols // HEAD_DIM
        keyval = acc_kv[...]
        keyval = jnp.concatenate(
            [keyval[i * rows : (i + 1) * rows] for i in range(HEAD_DIM // cols)], axis=1
        )
        filler = jnp.zeros((PACK_ROWS - batch - rows, HEAD_DIM), jnp.float32)
        packet = jnp.concatenate([acc_q[...], keyval, filler], axis=0).astype(jnp.bfloat16)
        for copy in range(packet_ref.shape[0]):
            packet_ref[copy] = packet


def project(hidden_in, w_query, w_keyval_t, copies):
    batch, width = hidden_in.shape
    cols = w_keyval_t.shape[0]
    steps = 2
    chunk = width // steps
    return pl.pallas_call(
        project_kernel,
        grid=(steps,),
        in_specs=[
            pl.BlockSpec((batch, chunk), lambda k: (0, k)),
            pl.BlockSpec((chunk, HEAD_DIM), lambda k: (k, 0)),
            pl.BlockSpec((cols, chunk), lambda k: (0, k)),
        ],
        out_specs=whole(),
        out_shape=vmem_out((copies, PACK_ROWS, HEAD_DIM), jnp.bfloat16),
        scratch_shapes=[
            pltpu.VMEM((batch, HEAD_DIM), jnp.float32),
            pltpu.VMEM((batch, cols), jnp.float32),
        ],
        compiler_params=limit(8),
        interpret=INTERPRET,
        name="project",
    )(in_hbm(hidden_in), in_hbm(w_query), in_hbm(w_keyval_t))


def new_token(where_ref, own_ref, partner_ref, score_ref, value_ref):
    core, own_group, own_at = where_ref[0], where_ref[1], where_ref[2]
    batch = value_ref.shape[0]
    blocks = own_ref.shape[0] // NEAR
    group_chips = own_ref.shape[0] // (2 * KV_HEADS)
    halves = []
    for half in range(2):
        pieces = []
        for e in range(group_chips):
            chip = (half * KV_HEADS + own_group) * group_chips + e
            at = chip % NEAR * blocks + place_of(chip // NEAR, blocks)
            own = own_ref[at, batch:, :].astype(jnp.float32)
            partner = partner_ref[at, batch:, :].astype(jnp.float32)
            pieces += [jnp.where(core == 0, own, partner), jnp.where(core == 0, partner, own)]
        cols = HEAD_DIM // len(pieces)
        rows = batch * cols // HEAD_DIM
        parts = []
        for q in range(HEAD_DIM // cols):
            lanes = slice(q * cols, (q + 1) * cols)
            parts.append(jnp.concatenate([piece[:rows, lanes] for piece in pieces], axis=1))
        halves.append(jnp.concatenate(parts, axis=0))
    query = own_ref[own_at, :batch, :].astype(jnp.float32)
    score = jnp.sum(query * halves[0], axis=1, keepdims=True) * (1.0 / math.sqrt(HEAD_DIM))
    row = lax.broadcasted_iota(jnp.int32, (batch, HEAD_DIM), 0)
    lane = lax.broadcasted_iota(jnp.int32, (batch, HEAD_DIM), 1)
    score_ref[...] = jnp.sum(jnp.where(row == lane, score, 0.0), axis=0, keepdims=True)
    value_ref[...] = halves[1]


def attend_kernel(where_ref, lengths_ref, own_ref, partner_ref, key_ref, value_ref,
                  mine_ref, theirs_ref, level_ref, level_theirs_ref, score_ref, new_value_ref,
                  q_scr, s_scr, o_scr, level_scr, keys_scr, values_scr, sems):
    blocks = own_ref.shape[0] // NEAR
    batch, ctx_dev, _ = key_ref.shape
    group = CORES * NEAR
    pack = group * batch
    parts = batch // STEP_ROWS
    order = block_order(blocks)
    f32, bf16 = jnp.float32, jnp.bfloat16

    def copy_of(kind, part):
        rows = pl.ds(part * STEP_ROWS, STEP_ROWS)
        source, target = ((key_ref, keys_scr), (value_ref, values_scr))[kind]
        return pltpu.make_async_copy(source.at[rows], target.at[rows], sems.at[kind, part])

    for kind in range(2):
        for part in range(parts):
            copy_of(kind, part).start()

    for g in range(blocks):
        for c, ref in enumerate((own_ref, partner_ref)):
            for i in range(NEAR):
                start = g * pack + c * NEAR + i
                tile = ref[i * blocks + g, :batch, :].astype(f32)
                q_scr[pl.ds(start, batch, stride=group), :] = tile
    for g in range(blocks):
        rows = slice(g * pack, (g + 1) * pack)
        q_scr[rows, :] = q_scr[rows, :].T
    new_token(where_ref, own_ref, partner_ref, score_ref, new_value_ref)

    lane_row = lax.broadcasted_iota(jnp.int32, (HEAD_DIM, pack), 1) // group
    s_scr[...] = jnp.zeros_like(s_scr)

    def score_part(part, carry):
        copy_of(0, part).wait()
        for g in range(blocks):
            columns = slice(order[g] * HEAD_DIM, (order[g] + 1) * HEAD_DIM)
            query = q_scr[g * pack : (g + 1) * pack, :]
            total = s_scr[g]
            for j in range(0, STEP_ROWS, 2):
                b = part * STEP_ROWS + j
                keys = jnp.concatenate(
                    [keys_scr[b, :, columns], keys_scr[b + 1, :, columns]], axis=1
                )
                picked = jnp.concatenate(
                    [
                        jnp.where(lane_row == b, query, 0.0).astype(bf16),
                        jnp.where(lane_row == b + 1, query, 0.0).astype(bf16),
                    ],
                    axis=0,
                )
                total += jnp.dot(keys, picked, preferred_element_type=f32)
            s_scr[g] = total
        return carry

    lax.fori_loop(0, parts, score_part, 0)

    level_scr[...] = jnp.full(level_scr.shape, EMPTY, f32)
    slot = lax.broadcasted_iota(jnp.int32, (ctx_dev, pack), 0)
    cached = jnp.zeros((1, pack), jnp.int32)
    for b in range(batch):
        cached = jnp.where(lane_row[:1] == b, lengths_ref[b] - where_ref[3], cached)
    used = slot < cached
    for g in range(blocks):
        scores = jnp.where(used, s_scr[g] * (1.0 / math.sqrt(HEAD_DIM)), EMPTY)
        top = jnp.max(scores, axis=0, keepdims=True)
        weights = jnp.where(used, jnp.exp(scores - top), 0.0)
        total = jnp.sum(weights, axis=0, keepdims=True)
        some = total > 0
        safe = jnp.where(some, total, 1.0)
        level_scr[g : g + 1, :] = jnp.where(some, top + jnp.log(safe), EMPTY)
        s_scr[g] = (weights / safe).T

    def value_part(part, carry):
        copy_of(1, part).wait()
        for j in range(STEP_ROWS):
            b = part * STEP_ROWS + j
            start = pl.multiple_of(b * group, group)
            for g in range(blocks):
                weights = s_scr[g, pl.ds(start, group), :].astype(bf16)
                columns = slice(order[g] * HEAD_DIM, (order[g] + 1) * HEAD_DIM)
                values = values_scr[b, :, columns]
                out = jnp.dot(weights, values, preferred_element_type=f32)
                o_scr[pl.ds(g * pack + start, group), :] = out
        return carry

    lax.fori_loop(0, parts, value_part, 0)

    level_scr[...] = level_scr[...].T
    for c, (ref, level) in enumerate(((mine_ref, level_ref), (theirs_ref, level_theirs_ref))):
        for i in range(NEAR):
            at = c * NEAR + i
            rows = slice(i * batch, (i + 1) * batch)
            level[rows, :] = level_scr[pl.ds(at, batch, stride=group), :]
            for g in range(blocks):
                tile = o_scr[pl.ds(g * pack + at, batch, stride=group), :]
                ref[i * blocks + g] = tile.astype(bf16)


def attend(where, lengths, own, partner, keys, values):
    batch, ctx_dev, _ = keys.shape
    chips = own.shape[0]
    blocks = chips // NEAR
    pack = CORES * NEAR * batch
    f32, bf16 = jnp.float32, jnp.bfloat16
    return pl.pallas_call(
        attend_kernel,
        grid_spec=pltpu.PrefetchScalarGridSpec(
            num_scalar_prefetch=2,
            grid=(1,),
            in_specs=[whole()] * 2 + [pl.BlockSpec(memory_space=pl.ANY)] * 2,
            out_specs=[whole()] * 6,
            scratch_shapes=[
                pltpu.VMEM((blocks * pack, HEAD_DIM), f32),
                pltpu.VMEM((blocks, ctx_dev, pack), f32),
                pltpu.VMEM((blocks * pack, HEAD_DIM), f32),
                pltpu.VMEM((pack, HEAD_DIM), f32),
                pltpu.VMEM(keys.shape, keys.dtype),
                pltpu.VMEM(values.shape, values.dtype),
                pltpu.SemaphoreType.DMA((2, batch // STEP_ROWS)),
            ],
        ),
        out_shape=[
            vmem_out((chips, batch, HEAD_DIM), bf16),
            vmem_out((chips, batch, HEAD_DIM), bf16),
            vmem_out((NEAR * batch, HEAD_DIM), f32),
            vmem_out((NEAR * batch, HEAD_DIM), f32),
            vmem_out((1, HEAD_DIM), f32),
            vmem_out((batch, HEAD_DIM), f32),
        ],
        compiler_params=limit(24),
        interpret=INTERPRET,
        name="attend",
    )(where, lengths, in_vmem(own), in_vmem(partner), in_hbm(keys), in_hbm(values))


def as_columns(*parts):
    count = sum(part.shape[0] for part in parts)
    filler = jnp.zeros((HEAD_DIM - count, HEAD_DIM), jnp.float32)
    return jnp.concatenate([*parts, filler], axis=0).T


def write_packet(ref, at, out, level):
    row = lax.broadcasted_iota(jnp.int32, (PACK_ROWS - out.shape[0], HEAD_DIM), 0)
    high = level.astype(jnp.bfloat16).astype(jnp.float32)
    middle = (level - high).astype(jnp.bfloat16).astype(jnp.float32)
    low = level - high - middle
    stats = jnp.where(row == 0, high, jnp.where(row == 1, middle, jnp.where(row == 2, low, 0.0)))
    ref[at] = jnp.concatenate([out, stats], axis=0).astype(jnp.bfloat16)


def read_levels(ref, batch, scr):
    for r in range(ref.shape[0]):
        stats = ref[r, batch:, :].astype(jnp.float32)
        scr[r : r + 1, :] = stats[0:1] + (stats[1:2] + stats[2:3])
    return scr[...]


def merge_cores_kernel(mine_ref, level_ref, got_ref, got_level_ref, out_ref):
    count, batch, _ = mine_ref.shape
    blocks = count // NEAR
    level, got = level_ref[...], got_level_ref[...]
    top = jnp.maximum(level, got)
    part_a, part_b = jnp.exp(level - top), jnp.exp(got - top)
    total = part_a + part_b
    part_a, part_b = part_a / total, part_b / total
    merged = as_columns(top + jnp.log(total))[:blocks]
    for i in range(NEAR):
        rows = slice(i * batch, (i + 1) * batch)
        levels = pltpu.roll(merged, (HEAD_DIM - i * batch) % HEAD_DIM, 1) if i else merged
        for k in range(blocks):
            r = i * blocks + k
            out = mine_ref[r].astype(jnp.float32) * part_a[rows, k : k + 1]
            out += got_ref[r].astype(jnp.float32) * part_b[rows, k : k + 1]
            write_packet(out_ref, r, out, levels[k : k + 1, :])


def merge_cores(mine, level, got, got_level):
    chips, batch, _ = mine.shape
    return pl.pallas_call(
        merge_cores_kernel,
        in_specs=[whole()] * 4,
        out_specs=whole(),
        out_shape=vmem_out((chips, PACK_ROWS, HEAD_DIM), jnp.bfloat16),
        compiler_params=limit(8),
        interpret=INTERPRET,
        name="merge_cores",
    )(in_vmem(mine), in_vmem(level), in_vmem(got), in_vmem(got_level))


def merge_near_kernel(batch, packet_ref, out_ref, level_scr):
    blocks = out_ref.shape[0]
    levels = read_levels(packet_ref, batch, level_scr)
    parts = [levels[i * blocks : (i + 1) * blocks] for i in range(NEAR)]
    top = functools.reduce(jnp.maximum, parts)
    parts = [jnp.exp(part - top) for part in parts]
    total = functools.reduce(jnp.add, parts)
    merged = top + jnp.log(total)
    columns = as_columns(*[part / total for part in parts])
    for k in range(blocks):
        out = 0.0
        for i in range(NEAR):
            r = i * blocks + k
            rows = packet_ref[r, :batch, :].astype(jnp.float32)
            out += rows * columns[:batch, r : r + 1]
        write_packet(out_ref, k, out, merged[k : k + 1, :])


def merge_near(packets, batch):
    count = packets.shape[0]
    return pl.pallas_call(
        functools.partial(merge_near_kernel, batch),
        in_specs=[whole()],
        out_specs=whole(),
        out_shape=vmem_out((count // NEAR, PACK_ROWS, HEAD_DIM), jnp.bfloat16),
        scratch_shapes=[pltpu.VMEM((count, HEAD_DIM), jnp.float32)],
        compiler_params=limit(8),
        interpret=INTERPRET,
        name="merge_near",
    )(in_vmem(packets))


def merge_far_kernel(packet_ref, score_ref, value_ref, out_ref, level_scr):
    batch = out_ref.shape[0]
    count = packet_ref.shape[0]
    levels = read_levels(packet_ref, batch, level_scr)
    score = score_ref[...]
    top = jnp.maximum(jnp.max(levels, axis=0, keepdims=True), score)
    parts, part_new = jnp.exp(levels - top), jnp.exp(score - top)
    total = jnp.sum(parts, axis=0, keepdims=True) + part_new
    columns = as_columns(parts / total, part_new / total)
    out = value_ref[...] * columns[:batch, count : count + 1]
    for r in range(count):
        out += packet_ref[r, :batch, :].astype(jnp.float32) * columns[:batch, r : r + 1]
    out_ref[...] = out.astype(out_ref.dtype)


def merge_far(packets, score_new, value_new):
    count = packets.shape[0]
    batch = value_new.shape[0]
    return pl.pallas_call(
        merge_far_kernel,
        in_specs=[whole()] * 3,
        out_specs=whole(),
        out_shape=vmem_out((batch, HEAD_DIM), jnp.bfloat16),
        scratch_shapes=[pltpu.VMEM((count, HEAD_DIM), jnp.float32)],
        compiler_params=limit(8),
        interpret=INTERPRET,
        name="merge_far",
    )(in_vmem(packets), in_vmem(score_new), in_vmem(value_new))


def output_kernel(where_ref, attended_ref, w_ref, mine_ref, theirs_ref):
    swap = where_ref[0] == 1
    attended = attended_ref[...]
    for i in range(NEAR):
        start = CORES * i * HEAD_DIM
        term = jnp.dot(
            attended,
            w_ref[:, start : start + CORES * HEAD_DIM],
            preferred_element_type=jnp.float32,
        )
        first, second = term[:, :HEAD_DIM], term[:, HEAD_DIM:]
        mine_ref[i, 0] = jnp.where(swap, second, first).astype(mine_ref.dtype)
        theirs_ref[i, 0] = jnp.where(swap, first, second).astype(theirs_ref.dtype)


def output_terms(where, attended, w_out):
    batch = attended.shape[0]
    rows, width = w_out.shape
    chunk = NEAR * CORES * HEAD_DIM
    blocks = width // chunk
    turn = block_order(blocks)[0]
    half = pl.BlockSpec((NEAR, 1, batch, HEAD_DIM), lambda s, *_: (0, s, 0, 0))
    return pl.pallas_call(
        output_kernel,
        grid_spec=pltpu.PrefetchScalarGridSpec(
            num_scalar_prefetch=1,
            grid=(blocks,),
            in_specs=[
                whole(),
                pl.BlockSpec((rows, chunk), lambda s, *_: (0, (s + turn) % blocks)),
            ],
            out_specs=[half, half],
        ),
        out_shape=[vmem_out((NEAR, blocks, batch, HEAD_DIM), jnp.bfloat16)] * 2,
        compiler_params=limit(8),
        interpret=INTERPRET,
        name="output_terms",
    )(where, in_vmem(attended), w_out)


def body(hidden_in, w_query, w_keyval, key_cache, value_cache, lengths, w_out):
    batch, ctx_dev, half_width = key_cache.shape
    shards = lax.axis_size("seq")
    index = lax.axis_index("seq")
    core = index % CORES
    chips = shards // CORES
    blocks = chips // NEAR
    heads = w_out.shape[0] // HEAD_DIM * shards
    group = heads // KV_HEADS
    f32, bf16 = jnp.float32, jnp.bfloat16

    chip = index // CORES
    own_at = chip % NEAR * blocks + place_of(chip // NEAR, blocks)
    where = jnp.stack([core, index // group, own_at, index * ctx_dev]).astype(jnp.int32)

    packet = project(hidden_in, w_query, w_keyval.T, blocks)
    far = exchange(packet, far_groups(shards))
    near = exchange(
        jnp.broadcast_to(far[None], (NEAR, *far.shape)).reshape(chips, *far.shape[1:]),
        near_groups(shards),
    )
    partner = to_partner(near, shards)

    mine, theirs, level, level_theirs, score_new, value_new = attend(
        where, lengths, near, partner, key_cache, value_cache
    )

    got = to_partner(theirs, shards)
    got_level = to_partner(level_theirs, shards)
    packets = exchange(merge_cores(mine, level, got, got_level), near_groups(shards))
    packets = exchange(merge_near(packets, batch), far_groups(shards))
    attended = merge_far(packets, score_new, value_new)

    mine, theirs = output_terms(where, attended, w_out)
    term = (mine.astype(f32) + to_partner(theirs, shards).astype(f32)).astype(bf16)
    arrived = exchange(term.reshape(chips, batch, -1), near_groups(shards))
    term = jnp.sum(arrived.reshape(NEAR, blocks, batch, -1).astype(f32), axis=0).astype(bf16)
    arrived = exchange(term, far_groups(shards))
    return jnp.sum(arrived.astype(f32), axis=0).astype(bf16)


def solution(mesh):
    placed = (
        P("replica", None),
        P(None, "seq"),
        P(None, "seq"),
        P("replica", "seq", None),
        P("replica", "seq", None),
        P("replica"),
        P("seq", None),
    )
    step = jax.shard_map(
        body, mesh=mesh, in_specs=placed, out_specs=P("replica", "seq"), check_vma=False
    )
    return step
```

```python
import functools
import math

import jax
import jax.numpy as jnp
from jax import lax
from jax.experimental import pallas as pl
from jax.experimental.pallas import tpu as pltpu
from jax.sharding import PartitionSpec as P


KV_HEADS = 8
HEAD_DIM = 128
CORES = 2
NEAR = 4
EMPTY = -1e30
FIRST_EIGHTH = 5
FIRST_NEAR = 2
NEAR_ORDER = [(q + FIRST_NEAR) % NEAR for q in range(NEAR)]
PACK_ROWS = 24
STEP_ROWS = 4
INTERPRET = False


def near_groups(shards):
    blocks = shards // CORES // NEAR
    return [
        [CORES * (NEAR * b + i) + c for i in NEAR_ORDER]
        for b in range(blocks)
        for c in range(CORES)
    ]


def block_order(blocks):
    return [(p + blocks * FIRST_EIGHTH // 8) % blocks for p in range(blocks)]


def place_of(chip, blocks):
    near = (chip % NEAR + NEAR - FIRST_NEAR) % NEAR
    return near * blocks + (chip // NEAR + blocks - blocks * FIRST_EIGHTH // 8) % blocks


def far_groups(shards):
    order = block_order(shards // CORES // NEAR)
    return [
        [CORES * (NEAR * b + i) + c for b in order] for i in range(NEAR) for c in range(CORES)
    ]


def exchange(x, groups):
    return lax.all_to_all(
        x, "seq", split_axis=0, concat_axis=0, axis_index_groups=groups, tiled=True
    )


def to_partner(x, shards):
    return lax.ppermute(x, "seq", [(i, i ^ 1) for i in range(shards)])


def in_vmem(x):
    return x if INTERPRET else pltpu.with_memory_space_constraint(x, pltpu.VMEM)


def in_hbm(x):
    return x if INTERPRET else pltpu.with_memory_space_constraint(x, pltpu.HBM)


def vmem_out(shape, dtype):
    return jax.ShapeDtypeStruct(shape, dtype) if INTERPRET else pltpu.VMEM(shape, dtype)


def hbm_out(shape, dtype):
    return jax.ShapeDtypeStruct(shape, dtype) if INTERPRET else pltpu.HBM(shape, dtype)


def whole():
    return pl.BlockSpec(memory_space=pltpu.VMEM)


def limit(mib):
    return pltpu.CompilerParams(vmem_limit_bytes=mib << 20)


def project_kernel(hidden_ref, w_query_ref, w_keyval_ref, packet_ref, acc_q, acc_kv):
    step = pl.program_id(0)

    @pl.when(step == 0)
    def _():
        acc_q[...] = jnp.zeros_like(acc_q)
        acc_kv[...] = jnp.zeros_like(acc_kv)

    hidden = hidden_ref[...]
    acc_q[...] += jnp.dot(hidden, w_query_ref[...], preferred_element_type=jnp.float32)
    acc_kv[...] += lax.dot_general(
        hidden, w_keyval_ref[...], (((1,), (1,)), ((), ())), preferred_element_type=jnp.float32
    )

    @pl.when(step == pl.num_programs(0) - 1)
    def _():
        batch, cols = acc_kv.shape
        rows = batch * cols // HEAD_DIM
        keyval = acc_kv[...]
        keyval = jnp.concatenate(
            [keyval[i * rows : (i + 1) * rows] for i in range(HEAD_DIM // cols)], axis=1
        )
        filler = jnp.zeros((PACK_ROWS - batch - rows, HEAD_DIM), jnp.float32)
        packet = jnp.concatenate([acc_q[...], keyval, filler], axis=0).astype(jnp.bfloat16)
        for copy in range(packet_ref.shape[0]):
            packet_ref[copy] = packet


def project(hidden_in, w_query, w_keyval_t, copies):
    batch, width = hidden_in.shape
    cols = w_keyval_t.shape[0]
    steps = 2
    chunk = width // steps
    return pl.pallas_call(
        project_kernel,
        grid=(steps,),
        in_specs=[
            pl.BlockSpec((batch, chunk), lambda k: (0, k)),
            pl.BlockSpec((chunk, HEAD_DIM), lambda k: (k, 0)),
            pl.BlockSpec((cols, chunk), lambda k: (0, k)),
        ],
        out_specs=whole(),
        out_shape=vmem_out((copies, PACK_ROWS, HEAD_DIM), jnp.bfloat16),
        scratch_shapes=[
            pltpu.VMEM((batch, HEAD_DIM), jnp.float32),
            pltpu.VMEM((batch, cols), jnp.float32),
        ],
        compiler_params=limit(8),
        interpret=INTERPRET,
        name="project",
    )(in_hbm(hidden_in), in_hbm(w_query), in_hbm(w_keyval_t))


def new_token(where_ref, own_ref, partner_ref, score_ref, value_ref):
    core, own_group, own_at = where_ref[0], where_ref[1], where_ref[2]
    batch = value_ref.shape[0]
    blocks = own_ref.shape[0] // NEAR
    group_chips = own_ref.shape[0] // (2 * KV_HEADS)
    halves = []
    for half in range(2):
        pieces = []
        for e in range(group_chips):
            chip = (half * KV_HEADS + own_group) * group_chips + e
            at = place_of(chip, blocks)
            own = own_ref[at, batch:, :].astype(jnp.float32)
            partner = partner_ref[at, batch:, :].astype(jnp.float32)
            pieces += [jnp.where(core == 0, own, partner), jnp.where(core == 0, partner, own)]
        cols = HEAD_DIM // len(pieces)
        rows = batch * cols // HEAD_DIM
        parts = []
        for q in range(HEAD_DIM // cols):
            lanes = slice(q * cols, (q + 1) * cols)
            parts.append(jnp.concatenate([piece[:rows, lanes] for piece in pieces], axis=1))
        halves.append(jnp.concatenate(parts, axis=0))
    query = own_ref[own_at, :batch, :].astype(jnp.float32)
    score = jnp.sum(query * halves[0], axis=1, keepdims=True) * (1.0 / math.sqrt(HEAD_DIM))
    row = lax.broadcasted_iota(jnp.int32, (batch, HEAD_DIM), 0)
    lane = lax.broadcasted_iota(jnp.int32, (batch, HEAD_DIM), 1)
    score_ref[...] = jnp.sum(jnp.where(row == lane, score, 0.0), axis=0, keepdims=True)
    value_ref[...] = halves[1]


def attend_kernel(where_ref, own_ref, partner_ref, key_ref, value_ref, lengths_ref,
                  mine_ref, theirs_ref, level_ref, level_theirs_ref, score_ref, new_value_ref,
                  q_scr, s_scr, o_scr, level_scr, keys_scr, values_scr, lengths_scr, sems,
                  lengths_sem):
    blocks = own_ref.shape[0] // NEAR
    batch, ctx_dev, _ = key_ref.shape
    group = CORES * NEAR
    pack = group * batch
    parts = batch // STEP_ROWS
    order = block_order(blocks)
    f32, bf16 = jnp.float32, jnp.bfloat16

    def copy_of(kind, part):
        rows = pl.ds(part * STEP_ROWS, STEP_ROWS)
        source, target = ((key_ref, keys_scr), (value_ref, values_scr))[kind]
        return pltpu.make_async_copy(source.at[rows], target.at[rows], sems.at[kind, part])

    lengths_copy = pltpu.make_async_copy(lengths_ref, lengths_scr, lengths_sem)
    lengths_copy.start()
    for kind in range(2):
        for part in range(parts):
            copy_of(kind, part).start()

    for g in range(blocks):
        for c, ref in enumerate((own_ref, partner_ref)):
            for i in range(NEAR):
                start = g * pack + c * NEAR + i
                tile = ref[i * blocks + g, :batch, :].astype(f32)
                q_scr[pl.ds(start, batch, stride=group), :] = tile
    for g in range(blocks):
        rows = slice(g * pack, (g + 1) * pack)
        q_scr[rows, :] = q_scr[rows, :].T
    new_token(where_ref, own_ref, partner_ref, score_ref, new_value_ref)

    lane_row = lax.broadcasted_iota(jnp.int32, (HEAD_DIM, pack), 1) // group
    s_scr[...] = jnp.zeros_like(s_scr)

    def score_part(part, carry):
        copy_of(0, part).wait()
        for g in range(blocks):
            columns = slice(order[g] * HEAD_DIM, (order[g] + 1) * HEAD_DIM)
            query = q_scr[g * pack : (g + 1) * pack, :]
            total = s_scr[g]
            for j in range(0, STEP_ROWS, 2):
                b = part * STEP_ROWS + j
                keys = jnp.concatenate(
                    [keys_scr[b, :, columns], keys_scr[b + 1, :, columns]], axis=1
                )
                picked = jnp.concatenate(
                    [
                        jnp.where(lane_row == b, query, 0.0).astype(bf16),
                        jnp.where(lane_row == b + 1, query, 0.0).astype(bf16),
                    ],
                    axis=0,
                )
                total += jnp.dot(keys, picked, preferred_element_type=f32)
            s_scr[g] = total
        return carry

    lax.fori_loop(0, parts, score_part, 0)

    level_scr[...] = jnp.full(level_scr.shape, EMPTY, f32)
    slot = lax.broadcasted_iota(jnp.int32, (ctx_dev, pack), 0)
    lengths_copy.wait()
    cached = jnp.zeros((1, pack), jnp.int32)
    for b in range(batch):
        cached = jnp.where(lane_row[:1] == b, lengths_scr[b] - where_ref[3], cached)
    used = slot < cached
    for g in range(blocks):
        scores = jnp.where(used, s_scr[g] * (1.0 / math.sqrt(HEAD_DIM)), EMPTY)
        top = jnp.max(scores, axis=0, keepdims=True)
        weights = jnp.where(used, jnp.exp(scores - top), 0.0)
        total = jnp.sum(weights, axis=0, keepdims=True)
        some = total > 0
        safe = jnp.where(some, total, 1.0)
        level_scr[g : g + 1, :] = jnp.where(some, top + jnp.log(safe), EMPTY)
        s_scr[g] = (weights / safe).T

    def value_part(part, carry):
        copy_of(1, part).wait()
        for j in range(STEP_ROWS):
            b = part * STEP_ROWS + j
            start = pl.multiple_of(b * group, group)
            for g in range(blocks):
                weights = s_scr[g, pl.ds(start, group), :].astype(bf16)
                columns = slice(order[g] * HEAD_DIM, (order[g] + 1) * HEAD_DIM)
                values = values_scr[b, :, columns]
                out = jnp.dot(weights, values, preferred_element_type=f32)
                o_scr[pl.ds(g * pack + start, group), :] = out
        return carry

    lax.fori_loop(0, parts, value_part, 0)

    level_scr[...] = level_scr[...].T
    for c, (ref, level) in enumerate(((mine_ref, level_ref), (theirs_ref, level_theirs_ref))):
        for i in range(NEAR):
            at = c * NEAR + i
            rows = slice(i * batch, (i + 1) * batch)
            level[rows, :] = level_scr[pl.ds(at, batch, stride=group), :]
            for g in range(blocks):
                tile = o_scr[pl.ds(g * pack + at, batch, stride=group), :]
                ref[i * blocks + g] = tile.astype(bf16)


def attend(where, lengths, own, partner, keys, values):
    batch, ctx_dev, _ = keys.shape
    chips = own.shape[0]
    blocks = chips // NEAR
    pack = CORES * NEAR * batch
    f32, bf16 = jnp.float32, jnp.bfloat16
    return pl.pallas_call(
        attend_kernel,
        grid_spec=pltpu.PrefetchScalarGridSpec(
            num_scalar_prefetch=1,
            grid=(1,),
            in_specs=[whole()] * 2 + [pl.BlockSpec(memory_space=pl.ANY)] * 3,
            out_specs=[whole()] * 6,
            scratch_shapes=[
                pltpu.VMEM((blocks * pack, HEAD_DIM), f32),
                pltpu.VMEM((blocks, ctx_dev, pack), f32),
                pltpu.VMEM((blocks * pack, HEAD_DIM), f32),
                pltpu.VMEM((pack, HEAD_DIM), f32),
                pltpu.VMEM(keys.shape, keys.dtype),
                pltpu.VMEM(values.shape, values.dtype),
                pltpu.SMEM(lengths.shape, lengths.dtype),
                pltpu.SemaphoreType.DMA((2, batch // STEP_ROWS)),
                pltpu.SemaphoreType.DMA,
            ],
        ),
        out_shape=[
            vmem_out((chips, batch, HEAD_DIM), bf16),
            vmem_out((chips, batch, HEAD_DIM), bf16),
            vmem_out((NEAR * batch, HEAD_DIM), f32),
            vmem_out((NEAR * batch, HEAD_DIM), f32),
            vmem_out((1, HEAD_DIM), f32),
            vmem_out((batch, HEAD_DIM), f32),
        ],
        compiler_params=limit(24),
        interpret=INTERPRET,
        name="attend",
    )(
        where,
        in_vmem(own),
        in_vmem(partner),
        in_hbm(keys),
        in_hbm(values),
        in_hbm(lengths),
    )


def as_columns(*parts):
    count = sum(part.shape[0] for part in parts)
    filler = jnp.zeros((HEAD_DIM - count, HEAD_DIM), jnp.float32)
    return jnp.concatenate([*parts, filler], axis=0).T


def write_packet(ref, at, out, level):
    row = lax.broadcasted_iota(jnp.int32, (PACK_ROWS - out.shape[0], HEAD_DIM), 0)
    high = level.astype(jnp.bfloat16).astype(jnp.float32)
    middle = (level - high).astype(jnp.bfloat16).astype(jnp.float32)
    low = level - high - middle
    stats = jnp.where(row == 0, high, jnp.where(row == 1, middle, jnp.where(row == 2, low, 0.0)))
    ref[at] = jnp.concatenate([out, stats], axis=0).astype(jnp.bfloat16)


def read_levels(ref, batch, scr):
    for r in range(ref.shape[0]):
        stats = ref[r, batch:, :].astype(jnp.float32)
        scr[r : r + 1, :] = stats[0:1] + (stats[1:2] + stats[2:3])
    return scr[...]


def merge_cores_kernel(mine_ref, level_ref, got_ref, got_level_ref, out_ref):
    count, batch, _ = mine_ref.shape
    blocks = count // NEAR
    level, got = level_ref[...], got_level_ref[...]
    top = jnp.maximum(level, got)
    part_a, part_b = jnp.exp(level - top), jnp.exp(got - top)
    total = part_a + part_b
    part_a, part_b = part_a / total, part_b / total
    merged = as_columns(top + jnp.log(total))[:blocks]
    for i in range(NEAR):
        rows = slice(i * batch, (i + 1) * batch)
        levels = pltpu.roll(merged, (HEAD_DIM - i * batch) % HEAD_DIM, 1) if i else merged
        for k in range(blocks):
            r = i * blocks + k
            out = mine_ref[r].astype(jnp.float32) * part_a[rows, k : k + 1]
            out += got_ref[r].astype(jnp.float32) * part_b[rows, k : k + 1]
            write_packet(out_ref, r, out, levels[k : k + 1, :])


def merge_cores(mine, level, got, got_level):
    chips, batch, _ = mine.shape
    return pl.pallas_call(
        merge_cores_kernel,
        in_specs=[whole()] * 4,
        out_specs=whole(),
        out_shape=vmem_out((chips, PACK_ROWS, HEAD_DIM), jnp.bfloat16),
        compiler_params=limit(8),
        interpret=INTERPRET,
        name="merge_cores",
    )(in_vmem(mine), in_vmem(level), in_vmem(got), in_vmem(got_level))


def merge_near_kernel(batch, packet_ref, out_ref, level_scr):
    blocks = out_ref.shape[0]
    levels = read_levels(packet_ref, batch, level_scr)
    parts = [levels[i * blocks : (i + 1) * blocks] for i in range(NEAR)]
    top = functools.reduce(jnp.maximum, parts)
    parts = [jnp.exp(part - top) for part in parts]
    total = functools.reduce(jnp.add, parts)
    merged = top + jnp.log(total)
    columns = as_columns(*[part / total for part in parts])
    for k in range(blocks):
        out = 0.0
        for i in range(NEAR):
            r = i * blocks + k
            rows = packet_ref[r, :batch, :].astype(jnp.float32)
            out += rows * columns[:batch, r : r + 1]
        write_packet(out_ref, k, out, merged[k : k + 1, :])


def merge_near(packets, batch):
    count = packets.shape[0]
    return pl.pallas_call(
        functools.partial(merge_near_kernel, batch),
        in_specs=[whole()],
        out_specs=whole(),
        out_shape=vmem_out((count // NEAR, PACK_ROWS, HEAD_DIM), jnp.bfloat16),
        scratch_shapes=[pltpu.VMEM((count, HEAD_DIM), jnp.float32)],
        compiler_params=limit(8),
        interpret=INTERPRET,
        name="merge_near",
    )(in_vmem(packets))


def merge_far_kernel(packet_ref, score_ref, value_ref, out_ref, level_scr):
    batch = out_ref.shape[0]
    count = packet_ref.shape[0]
    levels = read_levels(packet_ref, batch, level_scr)
    score = score_ref[...]
    top = jnp.maximum(jnp.max(levels, axis=0, keepdims=True), score)
    parts, part_new = jnp.exp(levels - top), jnp.exp(score - top)
    total = jnp.sum(parts, axis=0, keepdims=True) + part_new
    columns = as_columns(parts / total, part_new / total)
    out = value_ref[...] * columns[:batch, count : count + 1]
    for r in range(count):
        out += packet_ref[r, :batch, :].astype(jnp.float32) * columns[:batch, r : r + 1]
    out_ref[...] = out.astype(out_ref.dtype)


def merge_far(packets, score_new, value_new):
    count = packets.shape[0]
    batch = value_new.shape[0]
    return pl.pallas_call(
        merge_far_kernel,
        in_specs=[whole()] * 3,
        out_specs=whole(),
        out_shape=vmem_out((batch, HEAD_DIM), jnp.bfloat16),
        scratch_shapes=[pltpu.VMEM((count, HEAD_DIM), jnp.float32)],
        compiler_params=limit(8),
        interpret=INTERPRET,
        name="merge_far",
    )(in_vmem(packets), in_vmem(score_new), in_vmem(value_new))


def output_kernel(order, where_ref, attended_ref, w_ref, mine_ref, theirs_ref):
    swap = where_ref[0] == 1
    attended = attended_ref[...]
    for p, block in enumerate(order):
        for q, i in enumerate(NEAR_ORDER):
            start = (block * NEAR + i) * CORES * HEAD_DIM
            term = jnp.dot(
                attended,
                w_ref[:, start : start + CORES * HEAD_DIM],
                preferred_element_type=jnp.float32,
            )
            first, second = term[:, :HEAD_DIM], term[:, HEAD_DIM:]
            mine_ref[q, p] = jnp.where(swap, second, first).astype(mine_ref.dtype)
            theirs_ref[q, p] = jnp.where(swap, first, second).astype(theirs_ref.dtype)


def output_terms(where, attended, w_out):
    batch = attended.shape[0]
    blocks = w_out.shape[1] // (NEAR * CORES * HEAD_DIM)
    return pl.pallas_call(
        functools.partial(output_kernel, block_order(blocks)),
        grid_spec=pltpu.PrefetchScalarGridSpec(
            num_scalar_prefetch=1,
            grid=(1,),
            in_specs=[whole(), whole()],
            out_specs=[whole(), whole()],
        ),
        out_shape=[vmem_out((NEAR, blocks, batch, HEAD_DIM), jnp.bfloat16)] * 2,
        compiler_params=limit(8),
        interpret=INTERPRET,
        name="output_terms",
    )(where, in_vmem(attended), in_vmem(w_out))


def body(hidden_in, w_query, w_keyval, key_cache, value_cache, lengths, w_out):
    batch, ctx_dev, half_width = key_cache.shape
    shards = lax.axis_size("seq")
    index = lax.axis_index("seq")
    core = index % CORES
    chips = shards // CORES
    blocks = chips // NEAR
    heads = w_out.shape[0] // HEAD_DIM * shards
    group = heads // KV_HEADS
    f32, bf16 = jnp.float32, jnp.bfloat16

    chip = index // CORES
    own_at = place_of(chip, blocks)
    where = jnp.stack([core, index // group, own_at, index * ctx_dev]).astype(jnp.int32)

    packet = project(hidden_in, w_query, w_keyval.T, blocks)
    far = exchange(packet, far_groups(shards))
    near = exchange(
        jnp.broadcast_to(far[None], (NEAR, *far.shape)).reshape(chips, *far.shape[1:]),
        near_groups(shards),
    )
    partner = to_partner(near, shards)

    mine, theirs, level, level_theirs, score_new, value_new = attend(
        where, lengths, near, partner, key_cache, value_cache
    )

    got = to_partner(theirs, shards)
    got_level = to_partner(level_theirs, shards)
    packets = exchange(merge_cores(mine, level, got, got_level), near_groups(shards))
    packets = exchange(merge_near(packets, batch), far_groups(shards))
    attended = merge_far(packets, score_new, value_new)

    mine, theirs = output_terms(where, attended, w_out)
    term = (mine.astype(f32) + to_partner(theirs, shards).astype(f32)).astype(bf16)
    arrived = exchange(term.reshape(chips, batch, -1), near_groups(shards))
    term = jnp.sum(arrived.reshape(NEAR, blocks, batch, -1).astype(f32), axis=0).astype(bf16)
    arrived = exchange(term, far_groups(shards))
    return jnp.sum(arrived.astype(f32), axis=0).astype(bf16)


def solution(mesh):
    placed = (
        P("replica", None),
        P(None, "seq"),
        P(None, "seq"),
        P("replica", "seq", None),
        P("replica", "seq", None),
        P("replica"),
        P("seq", None),
    )
    step = jax.shard_map(
        body, mesh=mesh, in_specs=placed, out_specs=P("replica", "seq"), check_vma=False
    )
    return step
```

```python
import functools
import math

import jax
import jax.numpy as jnp
from jax import lax
from jax.experimental import pallas as pl
from jax.experimental.pallas import tpu as pltpu
from jax.sharding import PartitionSpec as P


KV_HEADS = 8
HEAD_DIM = 128
CORES = 2
NEAR = 4
EMPTY = -1e30
FIRST_EIGHTH = 4
FIRST_NEAR = 2
NEAR_ORDER = [(q + FIRST_NEAR) % NEAR for q in range(NEAR)]
PACK_ROWS = 24
STEP_ROWS = 4
INTERPRET = False


def near_groups(shards):
    blocks = shards // CORES // NEAR
    return [
        [CORES * (NEAR * b + i) + c for i in NEAR_ORDER]
        for b in range(blocks)
        for c in range(CORES)
    ]


def block_order(blocks):
    return [(p + blocks * FIRST_EIGHTH // 8) % blocks for p in range(blocks)]


def place_of(chip, blocks):
    near = (chip % NEAR + NEAR - FIRST_NEAR) % NEAR
    return near * blocks + (chip // NEAR + blocks - blocks * FIRST_EIGHTH // 8) % blocks


def far_groups(shards):
    order = block_order(shards // CORES // NEAR)
    return [
        [CORES * (NEAR * b + i) + c for b in order] for i in range(NEAR) for c in range(CORES)
    ]


def exchange(x, groups):
    return lax.all_to_all(
        x, "seq", split_axis=0, concat_axis=0, axis_index_groups=groups, tiled=True
    )


def to_partner(x, shards):
    return lax.ppermute(x, "seq", [(i, i ^ 1) for i in range(shards)])


def in_vmem(x):
    return x if INTERPRET else pltpu.with_memory_space_constraint(x, pltpu.VMEM)


def in_hbm(x):
    return x if INTERPRET else pltpu.with_memory_space_constraint(x, pltpu.HBM)


def vmem_out(shape, dtype):
    return jax.ShapeDtypeStruct(shape, dtype) if INTERPRET else pltpu.VMEM(shape, dtype)


def hbm_out(shape, dtype):
    return jax.ShapeDtypeStruct(shape, dtype) if INTERPRET else pltpu.HBM(shape, dtype)


def whole():
    return pl.BlockSpec(memory_space=pltpu.VMEM)


def limit(mib):
    return pltpu.CompilerParams(vmem_limit_bytes=mib << 20)


def project_kernel(hidden_ref, w_query_ref, w_keyval_ref, packet_ref, acc_q, acc_kv):
    step = pl.program_id(0)

    @pl.when(step == 0)
    def _():
        acc_q[...] = jnp.zeros_like(acc_q)
        acc_kv[...] = jnp.zeros_like(acc_kv)

    hidden = hidden_ref[...]
    acc_q[...] += jnp.dot(hidden, w_query_ref[...], preferred_element_type=jnp.float32)
    acc_kv[...] += lax.dot_general(
        hidden, w_keyval_ref[...], (((1,), (1,)), ((), ())), preferred_element_type=jnp.float32
    )

    @pl.when(step == pl.num_programs(0) - 1)
    def _():
        batch, cols = acc_kv.shape
        rows = batch * cols // HEAD_DIM
        keyval = acc_kv[...]
        keyval = jnp.concatenate(
            [keyval[i * rows : (i + 1) * rows] for i in range(HEAD_DIM // cols)], axis=1
        )
        filler = jnp.zeros((PACK_ROWS - batch - rows, HEAD_DIM), jnp.float32)
        packet = jnp.concatenate([acc_q[...], keyval, filler], axis=0).astype(jnp.bfloat16)
        for copy in range(packet_ref.shape[0]):
            packet_ref[copy] = packet


def project(hidden_in, w_query, w_keyval_t, copies):
    batch, width = hidden_in.shape
    cols = w_keyval_t.shape[0]
    steps = 2
    chunk = width // steps
    return pl.pallas_call(
        project_kernel,
        grid=(steps,),
        in_specs=[
            pl.BlockSpec((batch, chunk), lambda k: (0, k)),
            pl.BlockSpec((chunk, HEAD_DIM), lambda k: (k, 0)),
            pl.BlockSpec((cols, chunk), lambda k: (0, k)),
        ],
        out_specs=whole(),
        out_shape=vmem_out((copies, PACK_ROWS, HEAD_DIM), jnp.bfloat16),
        scratch_shapes=[
            pltpu.VMEM((batch, HEAD_DIM), jnp.float32),
            pltpu.VMEM((batch, cols), jnp.float32),
        ],
        compiler_params=limit(8),
        interpret=INTERPRET,
        name="project",
    )(in_hbm(hidden_in), in_hbm(w_query), in_hbm(w_keyval_t))


def new_token(where_ref, own_ref, partner_ref, score_ref, value_ref):
    core, own_group, own_at = where_ref[0], where_ref[1], where_ref[2]
    batch = value_ref.shape[0]
    blocks = own_ref.shape[0] // NEAR
    group_chips = own_ref.shape[0] // (2 * KV_HEADS)
    halves = []
    for half in range(2):
        pieces = []
        for e in range(group_chips):
            chip = (half * KV_HEADS + own_group) * group_chips + e
            at = place_of(chip, blocks)
            own = own_ref[at, batch:, :].astype(jnp.float32)
            partner = partner_ref[at, batch:, :].astype(jnp.float32)
            pieces += [jnp.where(core == 0, own, partner), jnp.where(core == 0, partner, own)]
        cols = HEAD_DIM // len(pieces)
        rows = batch * cols // HEAD_DIM
        parts = []
        for q in range(HEAD_DIM // cols):
            lanes = slice(q * cols, (q + 1) * cols)
            parts.append(jnp.concatenate([piece[:rows, lanes] for piece in pieces], axis=1))
        halves.append(jnp.concatenate(parts, axis=0))
    query = own_ref[own_at, :batch, :].astype(jnp.float32)
    score = jnp.sum(query * halves[0], axis=1, keepdims=True) * (1.0 / math.sqrt(HEAD_DIM))
    row = lax.broadcasted_iota(jnp.int32, (batch, HEAD_DIM), 0)
    lane = lax.broadcasted_iota(jnp.int32, (batch, HEAD_DIM), 1)
    score_ref[...] = jnp.sum(jnp.where(row == lane, score, 0.0), axis=0, keepdims=True)
    value_ref[...] = halves[1]


def attend_kernel(where_ref, own_ref, partner_ref, key_ref, value_ref, lengths_ref,
                  mine_ref, theirs_ref, level_ref, level_theirs_ref, score_ref, new_value_ref,
                  q_scr, s_scr, o_scr, level_scr, keys_scr, values_scr, lengths_scr, sems,
                  lengths_sem):
    blocks = own_ref.shape[0] // NEAR
    batch, ctx_dev, _ = key_ref.shape
    group = CORES * NEAR
    pack = group * batch
    parts = batch // STEP_ROWS
    order = block_order(blocks)
    f32, bf16 = jnp.float32, jnp.bfloat16

    def copy_of(kind, part):
        rows = pl.ds(part * STEP_ROWS, STEP_ROWS)
        source, target = ((key_ref, keys_scr), (value_ref, values_scr))[kind]
        return pltpu.make_async_copy(source.at[rows], target.at[rows], sems.at[kind, part])

    lengths_copy = pltpu.make_async_copy(lengths_ref, lengths_scr, lengths_sem)
    lengths_copy.start()
    for kind in range(2):
        for part in range(parts):
            copy_of(kind, part).start()

    for g in range(blocks):
        for c, ref in enumerate((own_ref, partner_ref)):
            for i in range(NEAR):
                start = g * pack + c * NEAR + i
                tile = ref[i * blocks + g, :batch, :].astype(f32)
                q_scr[pl.ds(start, batch, stride=group), :] = tile
    for g in range(blocks):
        rows = slice(g * pack, (g + 1) * pack)
        q_scr[rows, :] = q_scr[rows, :].T
    new_token(where_ref, own_ref, partner_ref, score_ref, new_value_ref)

    lane_row = lax.broadcasted_iota(jnp.int32, (HEAD_DIM, pack), 1) // group
    s_scr[...] = jnp.zeros_like(s_scr)

    def score_part(part, carry):
        copy_of(0, part).wait()
        for g in range(blocks):
            columns = slice(order[g] * HEAD_DIM, (order[g] + 1) * HEAD_DIM)
            query = q_scr[g * pack : (g + 1) * pack, :]
            total = s_scr[g]
            for j in range(0, STEP_ROWS, 2):
                b = part * STEP_ROWS + j
                keys = jnp.concatenate(
                    [keys_scr[b, :, columns], keys_scr[b + 1, :, columns]], axis=1
                )
                picked = jnp.concatenate(
                    [
                        jnp.where(lane_row == b, query, 0.0).astype(bf16),
                        jnp.where(lane_row == b + 1, query, 0.0).astype(bf16),
                    ],
                    axis=0,
                )
                total += jnp.dot(keys, picked, preferred_element_type=f32)
            s_scr[g] = total
        return carry

    lax.fori_loop(0, parts, score_part, 0)

    level_scr[...] = jnp.full(level_scr.shape, EMPTY, f32)
    slot = lax.broadcasted_iota(jnp.int32, (ctx_dev, pack), 0)
    lengths_copy.wait()
    cached = jnp.zeros((1, pack), jnp.int32)
    for b in range(batch):
        cached = jnp.where(lane_row[:1] == b, lengths_scr[b] - where_ref[3], cached)
    used = slot < cached
    for g in range(blocks):
        scores = jnp.where(used, s_scr[g] * (1.0 / math.sqrt(HEAD_DIM)), EMPTY)
        top = jnp.max(scores, axis=0, keepdims=True)
        weights = jnp.where(used, jnp.exp(scores - top), 0.0)
        total = jnp.sum(weights, axis=0, keepdims=True)
        some = total > 0
        safe = jnp.where(some, total, 1.0)
        level_scr[g : g + 1, :] = jnp.where(some, top + jnp.log(safe), EMPTY)
        s_scr[g] = (weights / safe).T

    def value_part(part, carry):
        copy_of(1, part).wait()
        for j in range(STEP_ROWS):
            b = part * STEP_ROWS + j
            start = pl.multiple_of(b * group, group)
            for g in range(blocks):
                weights = s_scr[g, pl.ds(start, group), :].astype(bf16)
                columns = slice(order[g] * HEAD_DIM, (order[g] + 1) * HEAD_DIM)
                values = values_scr[b, :, columns]
                out = jnp.dot(weights, values, preferred_element_type=f32)
                o_scr[pl.ds(g * pack + start, group), :] = out
        return carry

    lax.fori_loop(0, parts, value_part, 0)

    level_scr[...] = level_scr[...].T
    for c, (ref, level) in enumerate(((mine_ref, level_ref), (theirs_ref, level_theirs_ref))):
        for i in range(NEAR):
            at = c * NEAR + i
            rows = slice(i * batch, (i + 1) * batch)
            level[rows, :] = level_scr[pl.ds(at, batch, stride=group), :]
            for g in range(blocks):
                tile = o_scr[pl.ds(g * pack + at, batch, stride=group), :]
                ref[i * blocks + g] = tile.astype(bf16)


def attend(where, lengths, own, partner, keys, values):
    batch, ctx_dev, _ = keys.shape
    chips = own.shape[0]
    blocks = chips // NEAR
    pack = CORES * NEAR * batch
    f32, bf16 = jnp.float32, jnp.bfloat16
    return pl.pallas_call(
        attend_kernel,
        grid_spec=pltpu.PrefetchScalarGridSpec(
            num_scalar_prefetch=1,
            grid=(1,),
            in_specs=[whole()] * 2 + [pl.BlockSpec(memory_space=pl.ANY)] * 3,
            out_specs=[whole()] * 6,
            scratch_shapes=[
                pltpu.VMEM((blocks * pack, HEAD_DIM), f32),
                pltpu.VMEM((blocks, ctx_dev, pack), f32),
                pltpu.VMEM((blocks * pack, HEAD_DIM), f32),
                pltpu.VMEM((pack, HEAD_DIM), f32),
                pltpu.VMEM(keys.shape, keys.dtype),
                pltpu.VMEM(values.shape, values.dtype),
                pltpu.SMEM(lengths.shape, lengths.dtype),
                pltpu.SemaphoreType.DMA((2, batch // STEP_ROWS)),
                pltpu.SemaphoreType.DMA,
            ],
        ),
        out_shape=[
            vmem_out((chips, batch, HEAD_DIM), bf16),
            vmem_out((chips, batch, HEAD_DIM), bf16),
            vmem_out((NEAR * batch, HEAD_DIM), f32),
            vmem_out((NEAR * batch, HEAD_DIM), f32),
            vmem_out((1, HEAD_DIM), f32),
            vmem_out((batch, HEAD_DIM), f32),
        ],
        compiler_params=limit(24),
        interpret=INTERPRET,
        name="attend",
    )(
        where,
        in_vmem(own),
        in_vmem(partner),
        in_hbm(keys),
        in_hbm(values),
        in_hbm(lengths),
    )


def as_columns(*parts):
    count = sum(part.shape[0] for part in parts)
    filler = jnp.zeros((HEAD_DIM - count, HEAD_DIM), jnp.float32)
    return jnp.concatenate([*parts, filler], axis=0).T


def write_packet(ref, at, out, level):
    row = lax.broadcasted_iota(jnp.int32, (PACK_ROWS - out.shape[0], HEAD_DIM), 0)
    high = level.astype(jnp.bfloat16).astype(jnp.float32)
    middle = (level - high).astype(jnp.bfloat16).astype(jnp.float32)
    low = level - high - middle
    stats = jnp.where(row == 0, high, jnp.where(row == 1, middle, jnp.where(row == 2, low, 0.0)))
    ref[at] = jnp.concatenate([out, stats], axis=0).astype(jnp.bfloat16)


def read_levels(ref, batch, scr):
    for r in range(ref.shape[0]):
        stats = ref[r, batch:, :].astype(jnp.float32)
        scr[r : r + 1, :] = stats[0:1] + (stats[1:2] + stats[2:3])
    return scr[...]


def merge_cores_kernel(mine_ref, level_ref, got_ref, got_level_ref, out_ref):
    count, batch, _ = mine_ref.shape
    blocks = count // NEAR
    level, got = level_ref[...], got_level_ref[...]
    top = jnp.maximum(level, got)
    part_a, part_b = jnp.exp(level - top), jnp.exp(got - top)
    total = part_a + part_b
    part_a, part_b = part_a / total, part_b / total
    merged = as_columns(top + jnp.log(total))[:blocks]
    for i in range(NEAR):
        rows = slice(i * batch, (i + 1) * batch)
        levels = pltpu.roll(merged, (HEAD_DIM - i * batch) % HEAD_DIM, 1) if i else merged
        for k in range(blocks):
            r = i * blocks + k
            out = mine_ref[r].astype(jnp.float32) * part_a[rows, k : k + 1]
            out += got_ref[r].astype(jnp.float32) * part_b[rows, k : k + 1]
            write_packet(out_ref, r, out, levels[k : k + 1, :])


def merge_cores(mine, level, got, got_level):
    chips, batch, _ = mine.shape
    return pl.pallas_call(
        merge_cores_kernel,
        in_specs=[whole()] * 4,
        out_specs=whole(),
        out_shape=vmem_out((chips, PACK_ROWS, HEAD_DIM), jnp.bfloat16),
        compiler_params=limit(8),
        interpret=INTERPRET,
        name="merge_cores",
    )(in_vmem(mine), in_vmem(level), in_vmem(got), in_vmem(got_level))


def merge_near_kernel(batch, packet_ref, out_ref, level_scr):
    blocks = out_ref.shape[0]
    levels = read_levels(packet_ref, batch, level_scr)
    parts = [levels[i * blocks : (i + 1) * blocks] for i in range(NEAR)]
    top = functools.reduce(jnp.maximum, parts)
    parts = [jnp.exp(part - top) for part in parts]
    total = functools.reduce(jnp.add, parts)
    merged = top + jnp.log(total)
    columns = as_columns(*[part / total for part in parts])
    for k in range(blocks):
        out = 0.0
        for i in range(NEAR):
            r = i * blocks + k
            rows = packet_ref[r, :batch, :].astype(jnp.float32)
            out += rows * columns[:batch, r : r + 1]
        write_packet(out_ref, k, out, merged[k : k + 1, :])


def merge_near(packets, batch):
    count = packets.shape[0]
    return pl.pallas_call(
        functools.partial(merge_near_kernel, batch),
        in_specs=[whole()],
        out_specs=whole(),
        out_shape=vmem_out((count // NEAR, PACK_ROWS, HEAD_DIM), jnp.bfloat16),
        scratch_shapes=[pltpu.VMEM((count, HEAD_DIM), jnp.float32)],
        compiler_params=limit(8),
        interpret=INTERPRET,
        name="merge_near",
    )(in_vmem(packets))


def merge_far_kernel(packet_ref, score_ref, value_ref, out_ref, level_scr):
    batch = out_ref.shape[0]
    count = packet_ref.shape[0]
    levels = read_levels(packet_ref, batch, level_scr)
    score = score_ref[...]
    top = jnp.maximum(jnp.max(levels, axis=0, keepdims=True), score)
    parts, part_new = jnp.exp(levels - top), jnp.exp(score - top)
    total = jnp.sum(parts, axis=0, keepdims=True) + part_new
    columns = as_columns(parts / total, part_new / total)
    out = value_ref[...] * columns[:batch, count : count + 1]
    for r in range(count):
        out += packet_ref[r, :batch, :].astype(jnp.float32) * columns[:batch, r : r + 1]
    out_ref[...] = out.astype(out_ref.dtype)


def merge_far(packets, score_new, value_new):
    count = packets.shape[0]
    batch = value_new.shape[0]
    return pl.pallas_call(
        merge_far_kernel,
        in_specs=[whole()] * 3,
        out_specs=whole(),
        out_shape=vmem_out((batch, HEAD_DIM), jnp.bfloat16),
        scratch_shapes=[pltpu.VMEM((count, HEAD_DIM), jnp.float32)],
        compiler_params=limit(8),
        interpret=INTERPRET,
        name="merge_far",
    )(in_vmem(packets), in_vmem(score_new), in_vmem(value_new))


def output_kernel(order, where_ref, attended_ref, w_ref, mine_ref, theirs_ref):
    swap = where_ref[0] == 1
    attended = attended_ref[...]
    for p, block in enumerate(order):
        for q, i in enumerate(NEAR_ORDER):
            start = (block * NEAR + i) * CORES * HEAD_DIM
            term = jnp.dot(
                attended,
                w_ref[:, start : start + CORES * HEAD_DIM],
                preferred_element_type=jnp.float32,
            )
            first, second = term[:, :HEAD_DIM], term[:, HEAD_DIM:]
            mine_ref[q, p] = jnp.where(swap, second, first).astype(mine_ref.dtype)
            theirs_ref[q, p] = jnp.where(swap, first, second).astype(theirs_ref.dtype)


def output_terms(where, attended, w_out):
    batch = attended.shape[0]
    blocks = w_out.shape[1] // (NEAR * CORES * HEAD_DIM)
    return pl.pallas_call(
        functools.partial(output_kernel, block_order(blocks)),
        grid_spec=pltpu.PrefetchScalarGridSpec(
            num_scalar_prefetch=1,
            grid=(1,),
            in_specs=[whole(), whole()],
            out_specs=[whole(), whole()],
        ),
        out_shape=[vmem_out((NEAR, blocks, batch, HEAD_DIM), jnp.bfloat16)] * 2,
        compiler_params=limit(8),
        interpret=INTERPRET,
        name="output_terms",
    )(where, in_vmem(attended), in_vmem(w_out))


def body(hidden_in, w_query, w_keyval, key_cache, value_cache, lengths, w_out):
    batch, ctx_dev, half_width = key_cache.shape
    shards = lax.axis_size("seq")
    index = lax.axis_index("seq")
    core = index % CORES
    chips = shards // CORES
    blocks = chips // NEAR
    heads = w_out.shape[0] // HEAD_DIM * shards
    group = heads // KV_HEADS
    f32, bf16 = jnp.float32, jnp.bfloat16

    chip = index // CORES
    own_at = place_of(chip, blocks)
    where = jnp.stack([core, index // group, own_at, index * ctx_dev]).astype(jnp.int32)

    packet = project(hidden_in, w_query, w_keyval.T, blocks)
    far = exchange(packet, far_groups(shards))
    near = exchange(
        jnp.broadcast_to(far[None], (NEAR, *far.shape)).reshape(chips, *far.shape[1:]),
        near_groups(shards),
    )
    partner = to_partner(near, shards)

    mine, theirs, level, level_theirs, score_new, value_new = attend(
        where, lengths, near, partner, key_cache, value_cache
    )

    got = to_partner(theirs, shards)
    got_level = to_partner(level_theirs, shards)
    packets = exchange(merge_cores(mine, level, got, got_level), near_groups(shards))
    packets = exchange(merge_near(packets, batch), far_groups(shards))
    attended = merge_far(packets, score_new, value_new)

    mine, theirs = output_terms(where, attended, w_out)
    term = (mine.astype(f32) + to_partner(theirs, shards).astype(f32)).astype(bf16)
    arrived = exchange(term.reshape(chips, batch, -1), near_groups(shards))
    term = jnp.sum(arrived.reshape(NEAR, blocks, batch, -1).astype(f32), axis=0).astype(bf16)
    arrived = exchange(term, far_groups(shards))
    return jnp.sum(arrived.astype(f32), axis=0).astype(bf16)


def solution(mesh):
    placed = (
        P("replica", None),
        P(None, "seq"),
        P(None, "seq"),
        P("replica", "seq", None),
        P("replica", "seq", None),
        P("replica"),
        P("seq", None),
    )
    step = jax.shard_map(
        body, mesh=mesh, in_specs=placed, out_specs=P("replica", "seq"), check_vma=False
    )
    return step
```
